128 devices in a mesh: seq: 64 (over z, y_hi, x, core), tp: 2 (over y_lo).
Axes of the slice: x: 4, y: 4 (y_hi: 2, y_lo: 2; y = y_hi * 2 + y_lo), z: 4, core: 2. Of those that a mesh axis runs over, the one named last changes fastest.
Arguments:
- mixer_input: bfloat16 [32768, 3072], P('seq', 'tp'), may hold values from -6 to 6
- state_write: bfloat16 [32768, 128], P('seq'), may hold values from -2 to 2
- state_read: bfloat16 [32768, 128], P('seq'), may hold values from -2 to 2
- step_size: float32 [32768, 48], P('seq', 'tp'), may hold values from 0.05 to 0.5
- log_decay: float32 [32768, 48], P('seq', 'tp'), may hold values from -1.8 to 0, as said below
- skip_gain: float32 [48], P('tp'), may hold values from 0.5 to 2
- head_gain: float32 [3072], P('tp'), may hold values from 0.25 to 1.75
- mixer_out: bfloat16 [3072, 3072], P('tp'), may hold values from -0.109375 to 0.109375
- residual: bfloat16 [32768, 3072], P('seq', 'tp'), may hold values from -6 to 6
- attn_gain: float32 [3072], replicated, may hold values from 0.25 to 1.75
- qkv_weight: bfloat16 [3072, 3, 1536], P(None, None, 'tp'), may hold values from -2 to 2
Outputs:
- stream: bfloat16 [32768, 3072], P('seq', 'tp')
- attended: bfloat16 [32768, 1536], P('seq', 'tp')
The draws below stay inside these ranges and needn't reach their ends.
Inputs may be any that keep to these rules, and one draw needn't show every extreme that they name: `log_decay`: negative everywhere.
All inputs are finite; a program needn't handle non-finite values.
Results may differ from the reference program's by a relative error of at most 0.03.
Values may be sent and summed in bfloat16 or wider, within the bound.
A program may use at most 192 MiB of HBM per device.

```python
import math
import jax
import jax.numpy as jnp
from jax import lax

D = 3072
MHEADS = 48
MDIM = 64
STATE = 128
AHEADS = 16
AHD = 96
WINDOW = 2048
TOK_DEV = 512
TOKEN_POSITIONS = 32768
N_TP = 2


def draw_log_decay(key, part):
    random_keys_split = jax.random.split(key, 7)
    slow_share = 0.5
    slow = jax.random.bernoulli(random_keys_split[0], slow_share, (MHEADS,))
    slow_rate = jnp.exp(jax.random.uniform(random_keys_split[1], (MHEADS,), jnp.float32, math.log(0.05), math.log(0.5))) / TOKEN_POSITIONS
    fast_rate = jnp.exp(jax.random.uniform(random_keys_split[2], (MHEADS,), jnp.float32, math.log(1.0 / 50.0), math.log(1.0 / 20.0)))
    head_speed = jnp.where(slow, slow_rate, fast_rate)
    device_multiplier = jnp.repeat(jnp.exp(jax.random.uniform(random_keys_split[3], (TOKEN_POSITIONS // TOK_DEV, MHEADS), jnp.float32, -math.log(2.0), math.log(2.0))), TOK_DEV, axis=0)
    token_multiplier = jnp.exp(jax.random.uniform(random_keys_split[4], (TOKEN_POSITIONS, MHEADS), jnp.float32, -math.log(2.0), math.log(2.0)))
    spike_location = jax.random.randint(random_keys_split[5], (3,), 0, TOKEN_POSITIONS)
    spike_penalty = jax.random.uniform(random_keys_split[6], (3,), jnp.float32, 0.22, 0.51)
    sequence_place = jnp.arange(TOKEN_POSITIONS)
    spike_events = jnp.sum(jnp.where(sequence_place[None, :] == spike_location[:, None], spike_penalty[:, None], 0.0), axis=0)
    return (-(head_speed[None, :] * device_multiplier * token_multiplier + spike_events[:, None])).astype(jnp.float32)


def draw_qkv_weight(key, part):
    random_keys_split = jax.random.split(key, 1)
    embed_all = AHEADS * AHD
    base = jnp.clip(jax.random.normal(random_keys_split[0], (D, 3, embed_all), jnp.float32), -5.0, 5.0) * D ** (-0.5)
    return jnp.clip(base, -2.0, 2.0).astype(jnp.bfloat16)


def block_levels(rng, extent, pieces, smallest, high):
    factor_of, own = 1.0, jax.random.fold_in(rng, 6)
    for position, parts in pieces:
        draws = jnp.exp(jax.random.uniform(jax.random.fold_in(own, position), (parts,), jnp.float32, smallest / len(pieces), high / len(pieces)))
        factor_of = factor_of * jnp.repeat(draws, extent[position] // parts).reshape([-1 if axis == position else 1 for axis in range(len(extent))])
    return factor_of


def noise(rng, shape, deviation, limit, cuts=(), kind=jnp.bfloat16):
    array = deviation * jax.random.normal(rng, shape, jnp.float32)
    if cuts:
        array = array * block_levels(rng, shape, cuts, -0.22, 0.18)
    return jnp.clip(array, -limit, limit).astype(kind)


def setup_inputs(seed: int = 0) -> dict:
    key_list = jax.random.split(jax.random.key(seed), 12)
    return {
        "mixer_input": noise(key_list[0], (TOKEN_POSITIONS, MHEADS * MDIM), 1.0, 6.0, ((0, 64), (1, 2))),
        "state_write": noise(key_list[1], (TOKEN_POSITIONS, STATE), 0.3, 2.0, ((0, 64),)),
        "state_read": noise(key_list[2], (TOKEN_POSITIONS, STATE), 0.3, 2.0, ((0, 64),)),
        "step_size": jnp.clip(jnp.exp(math.log(0.5) - 2.3025851 * jax.random.uniform(key_list[3], (TOKEN_POSITIONS, MHEADS), jnp.float32) ** block_levels(key_list[3], (TOKEN_POSITIONS, MHEADS), ((0, 64), (1, 2)), -0.2, 0.2)), 0.05, 0.5),
        "log_decay": draw_log_decay(jax.random.fold_in(key_list[11], 71), 0),
        "skip_gain": jnp.clip(0.5 + 1.5 * jax.random.uniform(key_list[5], (MHEADS,), jnp.float32) ** block_levels(key_list[5], (MHEADS,), ((0, 2),), -0.2, 0.2), 0.5, 2.0),
        "head_gain": jnp.clip(1.0 + 0.15 * jax.random.normal(key_list[6], (MHEADS * MDIM,), jnp.float32), 0.25, 1.75),
        "mixer_out": noise(key_list[7], (MHEADS * MDIM, D), (MHEADS * MDIM) ** -0.5, 0.109375, ((0, 2),)),
        "residual": noise(key_list[8], (TOKEN_POSITIONS, D), 1.0, 6.0, ((0, 64), (1, 2))),
        "attn_gain": jnp.clip(1.0 + 0.15 * jax.random.normal(key_list[9], (D,), jnp.float32), 0.25, 1.75),
        "qkv_weight": draw_qkv_weight(jax.random.fold_in(key_list[11], 71), 0),
    }


EPSILON = 1e-05

def reference(mixer_input, state_write, state_read, step_size, log_decay, skip_gain, head_gain, mixer_out, residual, attn_gain, qkv_weight):
    span_len = min(TOK_DEV, 256)
    span_count = TOKEN_POSITIONS // span_len

    def blocked(tensor):
        return tensor.reshape((span_count, span_len) + tensor.shape[1:])

    def span_step(carry, blocks):
        inputs, write_rows, read_rows, step_rows, decays = blocks
        cumulative = jnp.cumsum(decays, axis=0)
        totals = cumulative[-1]
        values = inputs.astype(jnp.float32).reshape(span_len, MHEADS, MDIM)
        scaled = (step_rows[:, :, None] * values).astype(jnp.bfloat16)
        intersection = jnp.dot(read_rows, write_rows.T, preferred_element_type=jnp.float32)
        sequence_place = jnp.arange(span_len)
        causal = sequence_place[:, None] >= sequence_place[None, :]
        log_gaps = cumulative.T[:, :, None] - cumulative.T[:, None, :]
        mixing = (jnp.where(causal, jnp.exp(jnp.where(causal, log_gaps, 0.0)), 0.0) * intersection).astype(jnp.bfloat16)
        inner_part = jnp.einsum('hts,shp->thp', mixing.astype(jnp.float32), scaled.astype(jnp.float32))
        carried = jnp.exp(cumulative)[:, :, None] * jnp.einsum('tn,hpn->thp', read_rows.astype(jnp.float32), carry, precision=lax.Precision.HIGHEST)
        outputs = inner_part + carried + skip_gain[None, :, None] * values
        written = jnp.exp(totals[None, :] - cumulative)[:, :, None] * scaled.astype(jnp.float32)
        state_term = jnp.einsum('shp,sn->hpn', written, write_rows.astype(jnp.float32), precision=lax.Precision.HIGHEST)
        new_state = jnp.exp(totals)[:, None, None] * carry + state_term
        return (new_state, outputs)
    initial = jnp.zeros((MHEADS, MDIM, STATE), jnp.float32)
    final_state, outputs = lax.scan(span_step, initial, (blocked(mixer_input), blocked(state_write), blocked(state_read), blocked(step_size), blocked(log_decay)))
    head_outputs = outputs.reshape(TOKEN_POSITIONS, MHEADS, MDIM)
    inverse_rms = lax.rsqrt(lax.optimization_barrier(jnp.mean(head_outputs * head_outputs, axis=2, keepdims=True)) + EPSILON)
    normed = ((head_outputs * inverse_rms).reshape(TOKEN_POSITIONS, MHEADS * MDIM) * head_gain).astype(jnp.bfloat16)
    run_len = MHEADS * MDIM // N_TP
    total_sum = residual.astype(jnp.float32)
    for group_index in range(N_TP):
        partial_value = jnp.dot(normed[:, group_index * run_len:(group_index + 1) * run_len], mixer_out[group_index * run_len:(group_index + 1) * run_len], preferred_element_type=jnp.float32)
        total_sum = total_sum + lax.optimization_barrier(partial_value.astype(jnp.bfloat16)).astype(jnp.float32)
    stream = total_sum.astype(jnp.bfloat16)
    stream_wide = stream.astype(jnp.float32)
    normed_stream = (stream_wide * lax.rsqrt(lax.optimization_barrier(jnp.mean(stream_wide * stream_wide, axis=1, keepdims=True)) + EPSILON) * attn_gain).astype(jnp.bfloat16)
    embed_all = AHEADS * AHD
    projected = jnp.dot(normed_stream, qkv_weight.reshape(D, 3 * embed_all), preferred_element_type=jnp.float32).astype(jnp.bfloat16).reshape(TOKEN_POSITIONS, 3, embed_all)
    query_all = projected[:, 0].reshape(TOKEN_POSITIONS, AHEADS, AHD)
    padding = jnp.zeros((WINDOW, AHEADS, AHD), jnp.bfloat16)
    padded_keys = jnp.concatenate([padding, projected[:, 1].reshape(TOKEN_POSITIONS, AHEADS, AHD)], axis=0)
    padded_values = jnp.concatenate([padding, projected[:, 2].reshape(TOKEN_POSITIONS, AHEADS, AHD)], axis=0)

    def one_block(block_index):
        row_start = (block_index * TOK_DEV).astype(jnp.int32)
        queries = lax.dynamic_slice_in_dim(query_all, row_start, TOK_DEV, 0)
        key_part = lax.dynamic_slice_in_dim(padded_keys, row_start, TOK_DEV + WINDOW, 0)
        value_part = lax.dynamic_slice_in_dim(padded_values, row_start, TOK_DEV + WINDOW, 0)
        scores = jnp.einsum('thd,rhd->htr', queries.astype(jnp.float32), key_part.astype(jnp.float32)) * AHD ** (-0.5)
        query_pos = jnp.arange(TOK_DEV)
        key_pos = jnp.arange(TOK_DEV + WINDOW)
        first_valid = WINDOW - row_start
        allowed = (key_pos[None, :] > query_pos[:, None]) & (key_pos[None, :] <= query_pos[:, None] + WINDOW) & (key_pos[None, :] >= first_valid)
        masked = jnp.where(allowed[None], scores, -jnp.inf)
        peak = lax.optimization_barrier(jnp.max(masked, axis=2, keepdims=True))
        raised = jnp.exp(masked - peak)
        weights = (raised / lax.optimization_barrier(jnp.sum(raised, axis=2, keepdims=True))).astype(jnp.bfloat16)
        result = jnp.einsum('htr,rhd->thd', weights.astype(jnp.float32), value_part.astype(jnp.float32))
        return result.astype(jnp.bfloat16).reshape(TOK_DEV, embed_all)
    blocks_out = lax.map(one_block, jnp.arange(TOKEN_POSITIONS // TOK_DEV, dtype=jnp.int32))
    attended = blocks_out.reshape(TOKEN_POSITIONS, embed_all)
    return (stream, attended)
```

```python
import jax
import jax.numpy as jnp
from jax import lax
from jax.sharding import Mesh
from jax.experimental import pallas as pl
from jax.experimental.pallas import tpu as pltpu
from jax.sharding import PartitionSpec as P

AHD = 96
WINDOW = 2048
SEQ = ("seq_0", "seq_1", "seq_2", "seq_3")


EPSILON = 1e-05


def filled_with(x, identity):
    return jax.tree.map(
        lambda a, e: jnp.broadcast_to(jnp.asarray(e, a.dtype), a.shape), x, identity
    )


def carried_in(x, axes, combine, identity):
    before = start = filled_with(x, identity)
    running = x
    for axis in reversed(axes):
        size, position = (lax.axis_size(axis), lax.axis_index(axis))
        pieces = jax.tree.map(
            lambda part, kind: lax.all_gather(part.astype(kind), axis),
            running,
            jax.tree.map(lambda a: jnp.bfloat16 if a.dtype == jnp.float32 else a.dtype, x),
        )
        inside, running = (start, start)
        for k in range(size):
            passed = k < position
            running = combine(
                running, jax.tree.map(lambda part, own: part[k].astype(own.dtype), pieces, x)
            )
            inside = jax.tree.map(lambda new, old: jnp.where(passed, new, old), running, inside)
        before = combine(inside, before)
    return before


def split_up(x, dim, size):
    lengths = x.shape
    pieces = x.reshape(*lengths[:dim], size, lengths[dim] // size, *lengths[dim + 1 :])
    return jnp.moveaxis(pieces, dim, 0)


def sum_at_owner(x, axis, dim):
    pieces = split_up(x, dim, lax.axis_size(axis))
    arrived = lax.all_to_all(pieces, axis, split_axis=0, concat_axis=0, tiled=True)
    return arrived.astype(jnp.float32).sum(axis=0)


def from_everyone(x, axis):
    size = lax.axis_size(axis)
    return lax.all_to_all(jnp.broadcast_to(x[None], (size, *x.shape)), axis, 0, 0, tiled=True)


def over_copies(x, axis):
    everything = from_everyone(x, axis)
    return jnp.sum(everything, axis=0)


def joined_along(pieces, dim):
    pieces = jnp.moveaxis(pieces, 0, dim)
    lengths = pieces.shape
    return pieces.reshape(*lengths[:dim], lengths[dim] * lengths[dim + 1], *lengths[dim + 2 :])


def gathered_copies(x, axis, dim):
    return joined_along(from_everyone(x, axis), dim)


def shifted(x, axis, by):
    size = lax.axis_size(axis)
    pairs = [(i, i + by) for i in range(size) if 0 <= i + by < size]
    return lax.ppermute(x, axis, pairs)


MESH = pl.DeviceIdType.MESH
F32 = jnp.float32
BF16 = jnp.bfloat16
NEG = -1e30
LOG2E = 1.4426950408889634


def attn_kernel(proj_ref, out_ref, own, buf, knat, osend, oland, send_sem, recv_sem,
                hsend_sem, hrecv_sem, osend_sem, orecv_sem):
    z = lax.axis_index("seq_0")
    yh = lax.axis_index("seq_1")
    xx = lax.axis_index("seq_2")
    cc = lax.axis_index("seq_3")
    g = xx * 2 + cc
    row = z * 2 + yh
    nrow = lax.rem(row + 1, 8)
    prow = lax.rem(row + 7, 8)
    hd = 96
    tok = 512

    def at_group(j):
        return {"seq_2": j // 2, "seq_3": lax.rem(j, 2)}

    def at_row(r):
        return {"seq_0": r // 2, "seq_1": lax.rem(r, 2)}

    barrier = pltpu.get_barrier_semaphore()
    for d in range(1, 8):
        pl.semaphore_signal(barrier, inc=1, device_id=at_group(lax.rem(g + d, 8)), device_id_type=MESH)
    pl.semaphore_signal(barrier, inc=1, device_id=at_row(nrow), device_id_type=MESH)
    pl.semaphore_signal(barrier, inc=1, device_id=at_row(prow), device_id_type=MESH)
    for i in range(3):
        own[i] = proj_ref[:, i * 768:(i + 1) * 768].T
    pl.semaphore_wait(barrier, 9)

    def head(j):
        return pl.ds(pl.multiple_of(j * hd, 32), hd)

    def block_copy(d):
        j = lax.rem(g + d, 8)
        return pltpu.make_async_remote_copy(
            src_ref=own.at[:, head(j), :],
            dst_ref=buf.at[4 + g],
            send_sem=send_sem.at[d],
            recv_sem=recv_sem.at[g],
            device_id=at_group(j), device_id_type=MESH)

    def arrival(b):
        return pltpu.make_async_copy(buf.at[4 + b], buf.at[4 + b], recv_sem.at[b])

    def halo_copy(i):
        return pltpu.make_async_remote_copy(
            src_ref=buf.at[8 + i, pl.ds(1, 2)],
            dst_ref=buf.at[i, pl.ds(1, 2)],
            send_sem=hsend_sem.at[i],
            recv_sem=hrecv_sem.at[i],
            device_id=at_row(nrow), device_id_type=MESH)

    for d in (4, 5, 3, 2, 6, 1, 7):
        block_copy(d).start()
    buf[4 + g] = own[:, head(g), :]

    def arrived(b):
        @pl.when(b != g)
        def _():
            arrival(b).wait()
        knat[4 + b] = buf[4 + b, 1].T

    for b in range(4, 8):
        arrived(b)

        @pl.when(row < 7)
        def _(i=b - 4):
            halo_copy(i).start()
    for b in range(4):
        arrived(b)

    scale = (hd ** -0.5) * LOG2E
    spos = lax.broadcasted_iota(jnp.int32, (tok, tok), 0)
    tpos = lax.broadcasted_iota(jnp.int32, (tok, tok), 1)
    causal = spos <= tpos

    def one_block(step, _):
        b = jnp.where(step < 4, 4 + step, 7 - step)

        @pl.when(jnp.logical_and(step >= 4, row > 0))
        def _():
            halo_copy(b).wait_recv()
            knat[b] = buf[b, 1].T

        qt = buf[4 + b, 0]
        s_diag = jnp.dot(knat[4 + b], qt, preferred_element_type=F32)
        has_far = jnp.logical_or(step < 4, row > 0)
        s_far = jnp.dot(knat[b], qt, preferred_element_type=F32)
        s = jnp.where(causal, s_diag, jnp.where(has_far, s_far, NEG))
        m = jnp.max(s, axis=0, keepdims=True)
        p = jnp.exp2((s - m) * scale)
        l = jnp.sum(p, axis=0, keepdims=True)
        p_diag = jnp.where(causal, p, 0.0).astype(BF16)
        acc = jnp.dot(buf[4 + b, 2], p_diag, preferred_element_type=F32)
        p_far = jnp.where(causal, 0.0, p).astype(BF16)
        v_far = jnp.where(has_far, buf[b, 2], jnp.zeros((hd, tok), BF16))
        acc = acc + jnp.dot(v_far, p_far, preferred_element_type=F32)

        def mid(j, carry):
            m, l, acc = carry
            s = jnp.dot(knat[j], qt, preferred_element_type=F32)
            m_new = jnp.maximum(m, jnp.max(s, axis=0, keepdims=True))
            alpha = jnp.exp2((m - m_new) * scale)
            p = jnp.exp2((s - m_new) * scale)
            l = alpha * l + jnp.sum(p, axis=0, keepdims=True)
            acc = alpha * acc + jnp.dot(buf[j, 2], p.astype(BF16), preferred_element_type=F32)
            return m_new, l, acc

        first = jnp.where(row > 0, b + 1, jnp.maximum(b + 1, 4))
        m, l, acc = lax.fori_loop(first, b + 4, mid, (m, l, acc))
        osend[b] = (acc / l).astype(BF16)

        @pl.when(b != g)
        def _():
            out_copy(b).start()
        return 0

    def out_copy(b):
        return pltpu.make_async_remote_copy(
            src_ref=osend.at[b],
            dst_ref=oland.at[g],
            send_sem=osend_sem.at[b],
            recv_sem=orecv_sem.at[g],
            device_id=at_group(b), device_id_type=MESH)

    @pl.when(row == 0)
    def _():
        for i in range(4):
            knat[i] = jnp.zeros((tok, hd), BF16)
    lax.fori_loop(0, 8, one_block, 0)
    oland[g] = osend[g]
    for b in range(8):
        @pl.when(b != g)
        def _(b=b):
            pltpu.make_async_copy(oland.at[b], oland.at[b], orecv_sem.at[b]).wait()
    out_ref[...] = oland[...].reshape(8 * hd, tok).T
    for d in range(1, 8):
        block_copy(d).wait_send()
    for b in range(8):
        @pl.when(b != g)
        def _(b=b):
            out_copy(b).wait_send()

    @pl.when(row < 7)
    def _():
        for i in range(4):
            halo_copy(i).wait_send()


def attention(proj):
    V = pltpu.VMEM
    D = pltpu.SemaphoreType.DMA
    return pl.pallas_call(
        attn_kernel,
        name="attn",
        out_shape=jax.ShapeDtypeStruct((512, 768), BF16),
        in_specs=[pl.BlockSpec(memory_space=V)],
        out_specs=pl.BlockSpec(memory_space=V),
        scratch_shapes=[
            V((3, 768, 512), BF16), V((12, 3, 96, 512), BF16), V((12, 512, 96), BF16),
            V((8, 96, 512), BF16), V((8, 96, 512), BF16),
            D((8,)), D((8,)), D((4,)), D((4,)), D((8,)), D((8,)),
        ],
        compiler_params=pltpu.CompilerParams(
            collective_id=3, has_side_effects=True, vmem_limit_bytes=56 * 2**20),
    )(proj)


def span_terms(inputs, write_rows, read_rows, step_rows, decays, skip_gain):
    length, head_count = step_rows.shape
    head_dim = inputs.shape[1] // head_count
    cumulative = jnp.cumsum(decays, axis=0)
    totals = cumulative[-1]
    values = inputs.astype(jnp.float32).reshape(length, head_count, head_dim)
    scaled = (step_rows[:, :, None] * values).astype(jnp.bfloat16)
    intersection = jnp.dot(read_rows, write_rows.T, preferred_element_type=jnp.float32)
    sequence_place = jnp.arange(length)
    causal = sequence_place[:, None] >= sequence_place[None, :]
    log_gaps = cumulative.T[:, :, None] - cumulative.T[:, None, :]
    mixing = (
        jnp.where(causal, jnp.exp(jnp.where(causal, log_gaps, 0.0)), 0.0) * intersection
    ).astype(jnp.bfloat16)
    inner_part = jnp.einsum("hts,shp->thp", mixing, scaled, preferred_element_type=jnp.float32)
    local_part = inner_part + skip_gain[None, :, None] * values
    written = jnp.exp(totals[None, :] - cumulative)[:, :, None] * scaled.astype(jnp.float32)
    state_term = jnp.einsum(
        "shp,sn->hpn", written, write_rows.astype(jnp.float32), precision=lax.Precision.HIGHEST
    )
    return (local_part, state_term, totals, cumulative)


def join_states(earlier_pair, later_pair):
    return (
        earlier_pair[0] * later_pair[0],
        later_pair[0][:, None, None] * earlier_pair[1] + later_pair[1],
    )


def fold_spans(running, span_piece):
    state_term, totals = span_piece
    decay_run, state_run = running
    factor = jnp.exp(totals)
    return (
        (decay_run * factor, factor[:, None, None] * state_run + state_term),
        (decay_run, state_run),
    )


def on_device(
    mixer_input,
    state_write,
    state_read,
    step_size,
    log_decay,
    skip_gain,
    head_gain,
    mixer_out,
    residual,
    attn_gain,
    qkv_weight,
):
    tokens_dev = mixer_input.shape[0]
    head_count = step_size.shape[1]
    channels = mixer_input.shape[1]
    head_dim = channels // head_count
    span_len = min(tokens_dev, 256)
    span_count = tokens_dev // span_len

    def blocked(tensor):
        return tensor.reshape((span_count, span_len) + tensor.shape[1:])

    local_part, state_terms, totals, cumulative = jax.vmap(
        span_terms, in_axes=(0, 0, 0, 0, 0, None)
    )(
        blocked(mixer_input),
        blocked(state_write),
        blocked(state_read),
        blocked(step_size),
        blocked(log_decay),
        skip_gain,
    )
    identity_pair = (
        jnp.ones((head_count,), jnp.float32),
        jnp.zeros((head_count, head_dim, state_write.shape[1]), jnp.float32),
    )
    device_pair, before = lax.scan(fold_spans, identity_pair, (state_terms, totals))
    carry_in = carried_in(device_pair, SEQ, join_states, identity_pair)
    entering = before[0][:, :, None, None] * carry_in[1][None] + before[1]
    from_before = jnp.exp(cumulative)[..., None] * jnp.einsum(
        "ctn,chpn->cthp",
        blocked(state_read).astype(jnp.float32),
        entering,
        precision=lax.Precision.HIGHEST,
    )
    head_outputs = (local_part + from_before).reshape(tokens_dev, head_count, head_dim)
    inverse_rms = lax.rsqrt(jnp.mean(head_outputs * head_outputs, axis=2, keepdims=True) + EPSILON)
    normed = ((head_outputs * inverse_rms).reshape(tokens_dev, channels) * head_gain).astype(
        jnp.bfloat16
    )
    partial_value = jnp.dot(normed, mixer_out, preferred_element_type=jnp.float32)
    model_width = partial_value.shape[1]
    half_width = residual.shape[1]
    own_sum = sum_at_owner(partial_value.astype(jnp.bfloat16), "tp", 1)
    stream = (residual.astype(jnp.float32) + own_sum).astype(jnp.bfloat16)
    stream_wide = stream.astype(jnp.float32)
    squares = over_copies(jnp.sum(stream_wide * stream_wide, axis=1), "tp")
    gain_half = lax.dynamic_slice_in_dim(
        attn_gain, lax.axis_index("tp") * half_width, half_width, 0
    )
    normed_half = (
        stream_wide * lax.rsqrt(squares / model_width + EPSILON)[:, None] * gain_half
    ).astype(jnp.bfloat16)
    normed_stream = gathered_copies(normed_half, "tp", 1)
    weight = jnp.transpose(qkv_weight, (1, 0, 2))
    projected = jnp.concatenate(
        [jnp.dot(normed_stream, weight[i], preferred_element_type=jnp.float32).astype(jnp.bfloat16) for i in range(3)],
        axis=1,
    )
    pieces = attention(projected)
    return (stream, pieces)


def solution(mesh):
    torus = Mesh(
        mesh.devices.reshape(4, 2, 4, 2, mesh.shape["tp"]),
        ("seq_0", "seq_1", "seq_2", "seq_3", "tp"),
    )
    in_specs = (
        P(SEQ, "tp"),
        P(SEQ, None),
        P(SEQ, None),
        P(SEQ, "tp"),
        P(SEQ, "tp"),
        P("tp"),
        P("tp"),
        P("tp", None),
        P(SEQ, "tp"),
        P(),
        P(None, None, "tp"),
    )
    out_specs = (P(SEQ, "tp"), P(SEQ, "tp"))
    return jax.shard_map(
        on_device, mesh=torus, in_specs=in_specs, out_specs=out_specs, check_vma=False
    )
```

```python
import jax
import jax.numpy as jnp
from jax import lax
from jax.sharding import Mesh
from jax.experimental import pallas as pl
from jax.experimental.pallas import tpu as pltpu
from jax.sharding import PartitionSpec as P

AHD = 96
WINDOW = 2048
SEQ = ("seq_0", "seq_1", "seq_2", "seq_3")


EPSILON = 1e-05


def split_up(x, dim, size):
    lengths = x.shape
    pieces = x.reshape(*lengths[:dim], size, lengths[dim] // size, *lengths[dim + 1 :])
    return jnp.moveaxis(pieces, dim, 0)


def sum_at_owner(x, axis, dim):
    pieces = split_up(x, dim, lax.axis_size(axis))
    arrived = lax.all_to_all(pieces, axis, split_axis=0, concat_axis=0, tiled=True)
    return arrived.astype(jnp.float32).sum(axis=0)


def from_everyone(x, axis):
    size = lax.axis_size(axis)
    return lax.all_to_all(jnp.broadcast_to(x[None], (size, *x.shape)), axis, 0, 0, tiled=True)


def over_copies(x, axis):
    everything = from_everyone(x, axis)
    return jnp.sum(everything, axis=0)


def joined_along(pieces, dim):
    pieces = jnp.moveaxis(pieces, 0, dim)
    lengths = pieces.shape
    return pieces.reshape(*lengths[:dim], lengths[dim] * lengths[dim + 1], *lengths[dim + 2 :])


def gathered_copies(x, axis, dim):
    return joined_along(from_everyone(x, axis), dim)


MESH = pl.DeviceIdType.MESH
F32 = jnp.float32
BF16 = jnp.bfloat16
NEG = -1e30
LOG2E = 1.4426950408889634


def attn_kernel(proj_ref, out_ref, own, buf, knat, osend, oland, send_sem, recv_sem,
                hsend_sem, hrecv_sem, osend_sem, orecv_sem):
    z = lax.axis_index("seq_0")
    yh = lax.axis_index("seq_1")
    xx = lax.axis_index("seq_2")
    cc = lax.axis_index("seq_3")
    g = xx * 2 + cc
    row = z * 2 + yh
    nrow = lax.rem(row + 1, 8)
    prow = lax.rem(row + 7, 8)
    hd = 96
    tok = 512

    def at_group(j):
        return {"seq_2": j // 2, "seq_3": lax.rem(j, 2)}

    def at_row(r):
        return {"seq_0": r // 2, "seq_1": lax.rem(r, 2)}

    barrier = pltpu.get_barrier_semaphore()
    for d in range(1, 8):
        pl.semaphore_signal(barrier, inc=1, device_id=at_group(lax.rem(g + d, 8)), device_id_type=MESH)
    pl.semaphore_signal(barrier, inc=1, device_id=at_row(nrow), device_id_type=MESH)
    pl.semaphore_signal(barrier, inc=1, device_id=at_row(prow), device_id_type=MESH)
    for i in range(3):
        own[i] = proj_ref[:, i * 768:(i + 1) * 768].T
    pl.semaphore_wait(barrier, 9)

    def head(j):
        return pl.ds(pl.multiple_of(j * hd, 32), hd)

    def block_copy(d):
        j = lax.rem(g + d, 8)
        return pltpu.make_async_remote_copy(
            src_ref=own.at[:, head(j), :],
            dst_ref=buf.at[4 + g],
            send_sem=send_sem.at[d],
            recv_sem=recv_sem.at[g],
            device_id=at_group(j), device_id_type=MESH)

    def arrival(b):
        return pltpu.make_async_copy(buf.at[4 + b], buf.at[4 + b], recv_sem.at[b])

    def halo_copy(i):
        return pltpu.make_async_remote_copy(
            src_ref=buf.at[8 + i, pl.ds(1, 2)],
            dst_ref=buf.at[i, pl.ds(1, 2)],
            send_sem=hsend_sem.at[i],
            recv_sem=hrecv_sem.at[i],
            device_id=at_row(nrow), device_id_type=MESH)

    for d in (4, 5, 3, 2, 6, 1, 7):
        block_copy(d).start()
    buf[4 + g] = own[:, head(g), :]

    def arrived(b):
        @pl.when(b != g)
        def _():
            arrival(b).wait()
        knat[4 + b] = buf[4 + b, 1].T

    for b in range(4, 8):
        arrived(b)

        @pl.when(row < 7)
        def _(i=b - 4):
            halo_copy(i).start()
    for b in range(4):
        arrived(b)

    scale = (hd ** -0.5) * LOG2E
    spos = lax.broadcasted_iota(jnp.int32, (tok, tok), 0)
    tpos = lax.broadcasted_iota(jnp.int32, (tok, tok), 1)
    causal = spos <= tpos

    def one_block(step, _):
        b = jnp.where(step < 4, 4 + step, 7 - step)

        @pl.when(jnp.logical_and(step >= 4, row > 0))
        def _():
            halo_copy(b).wait_recv()
            knat[b] = buf[b, 1].T

        qt = buf[4 + b, 0]
        s_diag = jnp.dot(knat[4 + b], qt, preferred_element_type=F32)
        has_far = jnp.logical_or(step < 4, row > 0)
        s_far = jnp.dot(knat[b], qt, preferred_element_type=F32)
        s = jnp.where(causal, s_diag, jnp.where(has_far, s_far, NEG))
        m = jnp.max(s, axis=0, keepdims=True)
        p = jnp.exp2((s - m) * scale)
        l = jnp.sum(p, axis=0, keepdims=True)
        p_diag = jnp.where(causal, p, 0.0).astype(BF16)
        acc = jnp.dot(buf[4 + b, 2], p_diag, preferred_element_type=F32)
        p_far = jnp.where(causal, 0.0, p).astype(BF16)
        v_far = jnp.where(has_far, buf[b, 2], jnp.zeros((hd, tok), BF16))
        acc = acc + jnp.dot(v_far, p_far, preferred_element_type=F32)

        def mid(j, carry):
            m, l, acc = carry
            s = jnp.dot(knat[j], qt, preferred_element_type=F32)
            m_new = jnp.maximum(m, jnp.max(s, axis=0, keepdims=True))
            alpha = jnp.exp2((m - m_new) * scale)
            p = jnp.exp2((s - m_new) * scale)
            l = alpha * l + jnp.sum(p, axis=0, keepdims=True)
            acc = alpha * acc + jnp.dot(buf[j, 2], p.astype(BF16), preferred_element_type=F32)
            return m_new, l, acc

        first = jnp.where(row > 0, b + 1, jnp.maximum(b + 1, 4))
        m, l, acc = lax.fori_loop(first, b + 4, mid, (m, l, acc))
        osend[b] = (acc / l).astype(BF16)

        @pl.when(b != g)
        def _():
            out_copy(b).start()
        return 0

    def out_copy(b):
        return pltpu.make_async_remote_copy(
            src_ref=osend.at[b],
            dst_ref=oland.at[g],
            send_sem=osend_sem.at[b],
            recv_sem=orecv_sem.at[g],
            device_id=at_group(b), device_id_type=MESH)

    @pl.when(row == 0)
    def _():
        for i in range(4):
            knat[i] = jnp.zeros((tok, hd), BF16)
    lax.fori_loop(0, 8, one_block, 0)
    oland[g] = osend[g]
    for b in range(8):
        @pl.when(b != g)
        def _(b=b):
            pltpu.make_async_copy(oland.at[b], oland.at[b], orecv_sem.at[b]).wait()
    out_ref[...] = oland[...].reshape(8 * hd, tok).T
    for d in range(1, 8):
        block_copy(d).wait_send()
    for b in range(8):
        @pl.when(b != g)
        def _(b=b):
            out_copy(b).wait_send()

    @pl.when(row < 7)
    def _():
        for i in range(4):
            halo_copy(i).wait_send()


def attention(proj):
    V = pltpu.VMEM
    D = pltpu.SemaphoreType.DMA
    return pl.pallas_call(
        attn_kernel,
        name="attn",
        out_shape=jax.ShapeDtypeStruct((512, 768), BF16),
        in_specs=[pl.BlockSpec(memory_space=V)],
        out_specs=pl.BlockSpec(memory_space=V),
        scratch_shapes=[
            V((3, 768, 512), BF16), V((12, 3, 96, 512), BF16), V((12, 512, 96), BF16),
            V((8, 96, 512), BF16), V((8, 96, 512), BF16),
            D((8,)), D((8,)), D((4,)), D((4,)), D((8,)), D((8,)),
        ],
        compiler_params=pltpu.CompilerParams(
            collective_id=3, has_side_effects=True, vmem_limit_bytes=56 * 2**20),
    )(proj)

def parts_of(v, count):
    out = []
    for _ in range(count):
        piece = v.astype(BF16)
        out.append(piece)
        v = v - piece.astype(F32)
    return out


def one_hot(shape, per_lane, period=None):
    r = lax.broadcasted_iota(jnp.int32, shape, 0)
    c = lax.broadcasted_iota(jnp.int32, shape, 1)
    if period is not None:
        r = lax.rem(r, period)
    return jnp.where(r == c // per_lane, 1.0, 0.0).astype(BF16)


def mixer_kernel(x_ref, b_ref, c_ref, step_ref, ld_ref, skip_ref, hg_ref, n_ref,
                 u, ybuf, eexp, gexp, gt, s0, stage, rs, pref, dpre, rowst, rr, back, cin,
                 tst, tr, rtst, rtr,
                 a_send, a_recv, at_send, at_recv, r_send, r_recv, rt_send, rt_recv,
                 c_send, c_recv):
    z = lax.axis_index("seq_0")
    yh = lax.axis_index("seq_1")
    xx = lax.axis_index("seq_2")
    cc = lax.axis_index("seq_3")
    g = xx * 2 + cc
    row = z * 2 + yh
    nh, blk, wid = 24, 256, 1536

    def at_group(j):
        return {"seq_2": j // 2, "seq_3": lax.rem(j, 2)}

    def at_row(r):
        return {"seq_0": r // 2, "seq_1": lax.rem(r, 2)}

    barrier = pltpu.get_barrier_semaphore()
    for d in range(1, 8):
        pl.semaphore_signal(barrier, inc=1, device_id=at_group(lax.rem(g + d, 8)), device_id_type=MESH)
        pl.semaphore_signal(barrier, inc=1, device_id=at_row(lax.rem(row + d, 8)), device_id_type=MESH)

    def dot(a, b):
        return jnp.dot(a, b, preferred_element_type=F32)

    si = lax.broadcasted_iota(jnp.int32, (blk, blk), 0)
    ti = lax.broadcasted_iota(jnp.int32, (blk, blk), 1)
    upto = jnp.where(si <= ti, 1.0, 0.0).astype(BF16)
    wt = []
    for c in range(2):
        ld = ld_ref[:, c * blk:(c + 1) * blk]
        cat = jnp.concatenate(parts_of(ld, 3), axis=0)
        r = dot(cat, upto)
        gtc = (r[0:nh] + r[nh:2 * nh] + r[2 * nh:3 * nh]) * LOG2E
        gt[:, c * blk:(c + 1) * blk] = gtc
        wt.append(jnp.exp2(gtc[:, blk - 1:blk] - gtc))
    gtv = gt[...]
    g_col = gtv.T
    total = g_col[blk - 1:blk] + g_col[2 * blk - 1:2 * blk]
    tst[...] = jnp.zeros((8, 128), F32)
    tst[0:1, 0:nh] = total

    e3 = one_hot((3 * nh, wid), 64, nh)

    def expand(v, count=3):
        k = count * nh
        return dot(jnp.concatenate(parts_of(v, count), axis=1), e3[0:k] if count < 3 else e3)

    step_col = step_ref[...].T
    w_col = jnp.concatenate(wt, axis=1).T
    e_col = jnp.exp2(g_col)
    eexp[...] = expand(e_col)
    one3 = one_hot((3 * nh, nh * 128), 128, nh)
    gexp[...] = dot(jnp.concatenate(parts_of(g_col, 3), axis=1), one3)
    state = None
    for c in range(2):
        rows = slice(c * blk, (c + 1) * blk)
        uc = (expand(step_col[rows]) * x_ref[rows].astype(F32)).astype(BF16)
        u[rows] = uc
        wu = (expand(w_col[rows]) * uc.astype(F32)).astype(BF16)
        term = dot(b_ref[rows].T, wu)
        if c == 0:
            s0[...] = term
        else:
            state = eexp[2 * blk - 1:2 * blk] * s0[...] + term
    stage[...] = state.astype(BF16)
    pl.semaphore_wait(barrier, 14)

    def slice_of(j):
        return pl.ds(pl.multiple_of(j * 16, 16), 16)

    def a_copy(d):
        j = lax.rem(g + d, 8)
        return pltpu.make_async_remote_copy(
            src_ref=stage.at[slice_of(j)], dst_ref=rs.at[g],
            send_sem=a_send.at[d], recv_sem=a_recv.at[g],
            device_id=at_group(j), device_id_type=MESH)

    def at_copy(d):
        j = lax.rem(g + d, 8)
        return pltpu.make_async_remote_copy(
            src_ref=tst, dst_ref=tr.at[g],
            send_sem=at_send.at[d], recv_sem=at_recv.at[g],
            device_id=at_group(j), device_id_type=MESH)

    def r_copy(d):
        return pltpu.make_async_remote_copy(
            src_ref=rowst, dst_ref=rr.at[row],
            send_sem=r_send.at[d], recv_sem=r_recv.at[row],
            device_id=at_row(lax.rem(row + d, 8)), device_id_type=MESH)

    def rt_copy(d):
        return pltpu.make_async_remote_copy(
            src_ref=rtst, dst_ref=rtr.at[row],
            send_sem=rt_send.at[d], recv_sem=rt_recv.at[row],
            device_id=at_row(lax.rem(row + d, 8)), device_id_type=MESH)

    def c_copy(j):
        return pltpu.make_async_remote_copy(
            src_ref=back.at[j], dst_ref=cin.at[slice_of(g)],
            send_sem=c_send.at[j], recv_sem=c_recv.at[g],
            device_id=at_group(j), device_id_type=MESH)

    def landed(ref, sem):
        pltpu.make_async_copy(ref, ref, sem).wait()

    for d in range(1, 8):
        at_copy(d).start()
    for d in (4, 5, 3, 2, 6, 1, 7):
        a_copy(d).start()
    rs[g] = stage[slice_of(g), :]
    tr[g] = tst[...]

    causal = si >= ti

    def local_pairs(c, lo, hi):
        rows = slice(c * blk, (c + 1) * blk)
        cb = lax.dot_general(c_ref[rows], b_ref[rows], (((1,), (1,)), ((), ())),
                             preferred_element_type=F32)
        cb = jnp.where(causal, cb, 0.0)
        lane = lax.broadcasted_iota(jnp.int32, (blk, 128), 1)

        def pair(p, _):
            off = pl.multiple_of(p * 128, 128)
            up = u[rows, pl.ds(off, 128)]
            ys = []
            for k in range(2):
                h = p * 2 + k
                gc = gexp[rows, pl.ds(pl.multiple_of(h * 128, 128), 128)]
                gr = gt[pl.ds(h, 1), rows]
                gap = jnp.concatenate([gc, gc], axis=1) - gr
                m = (jnp.exp2(jnp.minimum(gap, 0.0)) * cb).astype(BF16)
                ys.append(dot(m, up))
            ybuf[rows, pl.ds(off, 128)] = jnp.where(lane < 64, ys[0], ys[1])
            return 0

        lax.fori_loop(lo, hi, pair, 0)

    local_pairs(0, 0, 12)

    for j in range(8):
        @pl.when(j != g)
        def _(j=j):
            landed(tr.at[j], at_recv.at[j])
            landed(rs.at[j], a_recv.at[j])
    e128 = one_hot((128, wid), 64)

    def table(ref):
        t = jnp.concatenate([ref[j, 0:1, :] for j in range(8)], axis=0)
        return t

    def spread(t):
        p = parts_of(t, 3)
        return dot(p[0], e128) + dot(p[1], e128) + dot(p[2], e128)

    tt = table(tr)
    dec = spread(jnp.exp2(tt))
    run = jnp.zeros((16, wid), F32)
    dr = jnp.ones((1, wid), F32)
    for j in range(8):
        pref[j] = run
        dpre[j:j + 1] = dr
        run = run * dec[j:j + 1] + rs[j].astype(F32)
        dr = dr * dec[j:j + 1]
    rowst[...] = run.astype(BF16)
    rtst[...] = jnp.broadcast_to(jnp.sum(tt, axis=0, keepdims=True), (8, 128))
    for d in range(1, 8):
        @pl.when(row + d < 8)
        def _(d=d):
            rt_copy(d).start()
            r_copy(d).start()

    local_pairs(1, 0, 8)

    for r in range(7):
        @pl.when(r < row)
        def _(r=r):
            landed(rtr.at[r], rt_recv.at[r])
            landed(rr.at[r], r_recv.at[r])
    rmask = lax.broadcasted_iota(jnp.int32, (8, 128), 0) < row
    rdec = spread(jnp.where(rmask, jnp.exp2(table(rtr)), 0.0))
    rc = jnp.zeros((16, wid), F32)
    for r in range(7):
        rc = jnp.where(r < row, rc * rdec[r:r + 1] + rr[r].astype(F32), rc)
    for j in range(8):
        back[j] = (pref[j] + dpre[j:j + 1] * rc).astype(BF16)
    for d in (4, 5, 3, 2, 6, 1, 7):
        c_copy(lax.rem(g + d, 8)).start()
    cin[slice_of(g), :] = back[g]

    local_pairs(1, 8, 12)

    skip = expand(jnp.broadcast_to(skip_ref[...], (8, nh)))[0:1]
    et = jnp.where(lax.broadcasted_iota(jnp.int32, (wid, nh), 0) // 64
                   == lax.broadcasted_iota(jnp.int32, (wid, nh), 1), 1.0, 0.0).astype(BF16)
    for j in range(8):
        @pl.when(j != g)
        def _(j=j):
            landed(cin.at[pl.ds(j * 16, 16)], c_recv.at[j])
    entering = cin[...].astype(F32)
    for c in range(2):
        rows = slice(c * blk, (c + 1) * blk)
        if c == 1:
            entering = eexp[blk - 1:blk] * entering + s0[...]
        y = ybuf[rows] + eexp[rows] * dot(c_ref[rows], entering.astype(BF16))
        y = y + skip * x_ref[rows].astype(F32)
        sq = parts_of(y * y, 2)
        ssum = dot(sq[0], et) + dot(sq[1], et)
        inv = lax.rsqrt(ssum * (1.0 / 64.0) + EPSILON)
        n_ref[rows] = (y * expand(inv) * hg_ref[...]).astype(BF16)

    for d in range(1, 8):
        at_copy(d).wait_send()
        a_copy(d).wait_send()
        c_copy(lax.rem(g + d, 8)).wait_send()

        @pl.when(row + d < 8)
        def _(d=d):
            rt_copy(d).wait_send()
            r_copy(d).wait_send()


def mixer(x, b, c, step, ld, skip, hg):
    V = pltpu.VMEM
    D = pltpu.SemaphoreType.DMA
    wid = 1536
    return pl.pallas_call(
        mixer_kernel,
        name="mixer",
        out_shape=jax.ShapeDtypeStruct((512, wid), BF16),
        in_specs=[pl.BlockSpec(memory_space=V)] * 7,
        out_specs=pl.BlockSpec(memory_space=V),
        scratch_shapes=[
            V((512, wid), BF16), V((512, wid), F32), V((512, wid), F32), V((512, 3072), F32),
            V((24, 512), F32), V((128, wid), F32), V((128, wid), BF16), V((8, 16, wid), BF16),
            V((8, 16, wid), F32), V((8, wid), F32), V((16, wid), BF16), V((8, 16, wid), BF16),
            V((8, 16, wid), BF16), V((128, wid), BF16),
            V((8, 128), F32), V((8, 8, 128), F32), V((8, 128), F32), V((8, 8, 128), F32),
        ] + [D((8,))] * 10,
        compiler_params=pltpu.CompilerParams(
            collective_id=1, has_side_effects=True, vmem_limit_bytes=60 * 2**20),
    )(x, b, c, step.T, ld.T, skip.reshape(1, 24), hg.reshape(1, wid))


def on_device(
    mixer_input,
    state_write,
    state_read,
    step_size,
    log_decay,
    skip_gain,
    head_gain,
    mixer_out,
    residual,
    attn_gain,
    qkv_weight,
):
    tokens_dev = mixer_input.shape[0]
    head_count = step_size.shape[1]
    channels = mixer_input.shape[1]
    head_dim = channels // head_count
    normed = mixer(mixer_input, state_write, state_read, step_size, log_decay, skip_gain, head_gain)
    partial_value = jnp.dot(normed, mixer_out, preferred_element_type=jnp.float32)
    model_width = partial_value.shape[1]
    half_width = residual.shape[1]
    own_sum = sum_at_owner(partial_value.astype(jnp.bfloat16), "tp", 1)
    stream = (residual.astype(jnp.float32) + own_sum).astype(jnp.bfloat16)
    stream_wide = stream.astype(jnp.float32)
    squares = over_copies(jnp.sum(stream_wide * stream_wide, axis=1), "tp")
    gain_half = lax.dynamic_slice_in_dim(
        attn_gain, lax.axis_index("tp") * half_width, half_width, 0
    )
    normed_half = (
        stream_wide * lax.rsqrt(squares / model_width + EPSILON)[:, None] * gain_half
    ).astype(jnp.bfloat16)
    normed_stream = gathered_copies(normed_half, "tp", 1)
    weight = jnp.transpose(qkv_weight, (1, 0, 2))
    projected = jnp.concatenate(
        [jnp.dot(normed_stream, weight[i], preferred_element_type=jnp.float32).astype(jnp.bfloat16) for i in range(3)],
        axis=1,
    )
    pieces = attention(projected)
    return (stream, pieces)


def solution(mesh):
    torus = Mesh(
        mesh.devices.reshape(4, 2, 4, 2, mesh.shape["tp"]),
        ("seq_0", "seq_1", "seq_2", "seq_3", "tp"),
    )
    in_specs = (
        P(SEQ, "tp"),
        P(SEQ, None),
        P(SEQ, None),
        P(SEQ, "tp"),
        P(SEQ, "tp"),
        P("tp"),
        P("tp"),
        P("tp", None),
        P(SEQ, "tp"),
        P(),
        P(None, None, "tp"),
    )
    out_specs = (P(SEQ, "tp"), P(SEQ, "tp"))
    return jax.shard_map(
        on_device, mesh=torus, in_specs=in_specs, out_specs=out_specs, check_vma=False
    )
```

```python
import jax
import jax.numpy as jnp
from jax import lax
from jax.sharding import Mesh
from jax.experimental import pallas as pl
from jax.experimental.pallas import tpu as pltpu
from jax.sharding import PartitionSpec as P

SEQ = ("seq_0", "seq_1", "seq_2", "seq_3")


EPSILON = 1e-05


MESH = pl.DeviceIdType.MESH
F32 = jnp.float32
BF16 = jnp.bfloat16
NEG = -1e30
LOG2E = 1.4426950408889634


def parts_of(v, count):
    out = []
    for _ in range(count):
        piece = v.astype(BF16)
        out.append(piece)
        v = v - piece.astype(F32)
    return out


def one_hot(shape, per_lane, period=None):
    r = lax.broadcasted_iota(jnp.int32, shape, 0)
    c = lax.broadcasted_iota(jnp.int32, shape, 1)
    if period is not None:
        r = lax.rem(r, period)
    return jnp.where(r == c // per_lane, 1.0, 0.0).astype(BF16)


def mixer_kernel(x_ref, b_ref, c_ref, step_ref, ld_ref, skip_ref, hg_ref, n_ref,
                 u, ybuf, eexp, gexp, gt, s0, stage, rs, pref, dpre, rowst, rr, back, cin,
                 tst, tr, rtst, rtr,
                 a_send, a_recv, at_send, at_recv, r_send, r_recv, rt_send, rt_recv,
                 c_send, c_recv):
    z = lax.axis_index("seq_0")
    yh = lax.axis_index("seq_1")
    xx = lax.axis_index("seq_2")
    cc = lax.axis_index("seq_3")
    g = xx * 2 + cc
    row = z * 2 + yh
    nh, blk, wid = 24, 256, 1536

    def at_group(j):
        return {"seq_2": j // 2, "seq_3": lax.rem(j, 2)}

    def at_row(r):
        return {"seq_0": r // 2, "seq_1": lax.rem(r, 2)}

    barrier = pltpu.get_barrier_semaphore()
    for d in range(1, 8):
        pl.semaphore_signal(barrier, inc=1, device_id=at_group(lax.rem(g + d, 8)), device_id_type=MESH)
        pl.semaphore_signal(barrier, inc=1, device_id=at_row(lax.rem(row + d, 8)), device_id_type=MESH)

    def dot(a, b):
        return jnp.dot(a, b, preferred_element_type=F32)

    si = lax.broadcasted_iota(jnp.int32, (blk, blk), 0)
    ti = lax.broadcasted_iota(jnp.int32, (blk, blk), 1)
    upto = jnp.where(si <= ti, 1.0, 0.0).astype(BF16)
    wt = []
    for c in range(2):
        ld = ld_ref[:, c * blk:(c + 1) * blk]
        cat = jnp.concatenate(parts_of(ld, 3), axis=0)
        r = dot(cat, upto)
        gtc = (r[0:nh] + r[nh:2 * nh] + r[2 * nh:3 * nh]) * LOG2E
        gt[:, c * blk:(c + 1) * blk] = gtc
        wt.append(jnp.exp2(gtc[:, blk - 1:blk] - gtc))
    gtv = gt[...]
    g_col = gtv.T
    total = g_col[blk - 1:blk] + g_col[2 * blk - 1:2 * blk]
    tst[...] = jnp.zeros((8, 128), F32)
    tst[0:1, 0:nh] = total

    e3 = one_hot((3 * nh, wid), 64, nh)

    def expand(v, count=3):
        k = count * nh
        return dot(jnp.concatenate(parts_of(v, count), axis=1), e3[0:k] if count < 3 else e3)

    step_col = step_ref[...].T
    w_col = jnp.concatenate(wt, axis=1).T
    e_col = jnp.exp2(g_col)
    eexp[...] = expand(e_col)
    one3 = one_hot((3 * nh, nh * 128), 128, nh)
    gexp[...] = dot(jnp.concatenate(parts_of(g_col, 3), axis=1), one3)
    state = None
    for c in range(2):
        rows = slice(c * blk, (c + 1) * blk)
        uc = (expand(step_col[rows]) * x_ref[rows].astype(F32)).astype(BF16)
        u[rows] = uc
        wu = (expand(w_col[rows]) * uc.astype(F32)).astype(BF16)
        term = dot(b_ref[rows].T, wu)
        if c == 0:
            s0[...] = term
        else:
            state = eexp[2 * blk - 1:2 * blk] * s0[...] + term
    stage[...] = state.astype(BF16)
    pl.semaphore_wait(barrier, 14)

    def slice_of(j):
        return pl.ds(pl.multiple_of(j * 16, 16), 16)

    def a_copy(d):
        j = lax.rem(g + d, 8)
        return pltpu.make_async_remote_copy(
            src_ref=stage.at[slice_of(j)], dst_ref=rs.at[g],
            send_sem=a_send.at[d], recv_sem=a_recv.at[g],
            device_id=at_group(j), device_id_type=MESH)

    def at_copy(d):
        j = lax.rem(g + d, 8)
        return pltpu.make_async_remote_copy(
            src_ref=tst, dst_ref=tr.at[g],
            send_sem=at_send.at[d], recv_sem=at_recv.at[g],
            device_id=at_group(j), device_id_type=MESH)

    def r_copy(d):
        return pltpu.make_async_remote_copy(
            src_ref=rowst, dst_ref=rr.at[row],
            send_sem=r_send.at[d], recv_sem=r_recv.at[row],
            device_id=at_row(lax.rem(row + d, 8)), device_id_type=MESH)

    def rt_copy(d):
        return pltpu.make_async_remote_copy(
            src_ref=rtst, dst_ref=rtr.at[row],
            send_sem=rt_send.at[d], recv_sem=rt_recv.at[row],
            device_id=at_row(lax.rem(row + d, 8)), device_id_type=MESH)

    def c_copy(j):
        return pltpu.make_async_remote_copy(
            src_ref=back.at[j], dst_ref=cin.at[slice_of(g)],
            send_sem=c_send.at[j], recv_sem=c_recv.at[g],
            device_id=at_group(j), device_id_type=MESH)

    def landed(ref, sem):
        pltpu.make_async_copy(ref, ref, sem).wait()

    for d in range(1, 8):
        at_copy(d).start()
    for d in (4, 5, 3, 2, 6, 1, 7):
        a_copy(d).start()
    rs[g] = stage[slice_of(g), :]
    tr[g] = tst[...]

    causal = si >= ti

    def local_pairs(c, lo, hi):
        rows = slice(c * blk, (c + 1) * blk)
        cb = lax.dot_general(c_ref[rows], b_ref[rows], (((1,), (1,)), ((), ())),
                             preferred_element_type=F32)
        cb = jnp.where(causal, cb, 0.0)
        lane = lax.broadcasted_iota(jnp.int32, (blk, 128), 1)

        def pair(p, _):
            off = pl.multiple_of(p * 128, 128)
            up = u[rows, pl.ds(off, 128)]
            ys = []
            for k in range(2):
                h = p * 2 + k
                gc = gexp[rows, pl.ds(pl.multiple_of(h * 128, 128), 128)]
                gr = gt[pl.ds(h, 1), rows]
                gap = jnp.concatenate([gc, gc], axis=1) - gr
                m = (jnp.exp2(jnp.minimum(gap, 0.0)) * cb).astype(BF16)
                ys.append(dot(m, up))
            ybuf[rows, pl.ds(off, 128)] = jnp.where(lane < 64, ys[0], ys[1])
            return 0

        lax.fori_loop(lo, hi, pair, 0)

    local_pairs(0, 0, 12)

    for j in range(8):
        @pl.when(j != g)
        def _(j=j):
            landed(tr.at[j], at_recv.at[j])
            landed(rs.at[j], a_recv.at[j])
    e128 = one_hot((128, wid), 64)

    def table(ref):
        t = jnp.concatenate([ref[j, 0:1, :] for j in range(8)], axis=0)
        return t

    def spread(t):
        p = parts_of(t, 3)
        return dot(p[0], e128) + dot(p[1], e128) + dot(p[2], e128)

    tt = table(tr)
    dec = spread(jnp.exp2(tt))
    run = jnp.zeros((16, wid), F32)
    dr = jnp.ones((1, wid), F32)
    for j in range(8):
        pref[j] = run
        dpre[j:j + 1] = dr
        run = run * dec[j:j + 1] + rs[j].astype(F32)
        dr = dr * dec[j:j + 1]
    rowst[...] = run.astype(BF16)
    rtst[...] = jnp.broadcast_to(jnp.sum(tt, axis=0, keepdims=True), (8, 128))
    for d in range(1, 8):
        @pl.when(row + d < 8)
        def _(d=d):
            rt_copy(d).start()
            r_copy(d).start()

    local_pairs(1, 0, 8)

    for r in range(7):
        @pl.when(r < row)
        def _(r=r):
            landed(rtr.at[r], rt_recv.at[r])
            landed(rr.at[r], r_recv.at[r])
    rmask = lax.broadcasted_iota(jnp.int32, (8, 128), 0) < row
    rdec = spread(jnp.where(rmask, jnp.exp2(table(rtr)), 0.0))
    rc = jnp.zeros((16, wid), F32)
    for r in range(7):
        rc = jnp.where(r < row, rc * rdec[r:r + 1] + rr[r].astype(F32), rc)
    for j in range(8):
        back[j] = (pref[j] + dpre[j:j + 1] * rc).astype(BF16)
    for d in (4, 5, 3, 2, 6, 1, 7):
        c_copy(lax.rem(g + d, 8)).start()
    cin[slice_of(g), :] = back[g]

    local_pairs(1, 8, 12)

    skip = expand(jnp.broadcast_to(skip_ref[...], (8, nh)))[0:1]
    et = jnp.where(lax.broadcasted_iota(jnp.int32, (wid, nh), 0) // 64
                   == lax.broadcasted_iota(jnp.int32, (wid, nh), 1), 1.0, 0.0).astype(BF16)
    for j in range(8):
        @pl.when(j != g)
        def _(j=j):
            landed(cin.at[pl.ds(j * 16, 16)], c_recv.at[j])
    entering = cin[...].astype(F32)
    for c in range(2):
        rows = slice(c * blk, (c + 1) * blk)
        if c == 1:
            entering = eexp[blk - 1:blk] * entering + s0[...]
        y = ybuf[rows] + eexp[rows] * dot(c_ref[rows], entering.astype(BF16))
        y = y + skip * x_ref[rows].astype(F32)
        sq = parts_of(y * y, 2)
        ssum = dot(sq[0], et) + dot(sq[1], et)
        inv = lax.rsqrt(ssum * (1.0 / 64.0) + EPSILON)
        n_ref[rows] = (y * expand(inv) * hg_ref[...]).astype(BF16)

    for d in range(1, 8):
        at_copy(d).wait_send()
        a_copy(d).wait_send()
        c_copy(lax.rem(g + d, 8)).wait_send()

        @pl.when(row + d < 8)
        def _(d=d):
            rt_copy(d).wait_send()
            r_copy(d).wait_send()


def mixer(x, b, c, step, ld, skip, hg):
    V = pltpu.VMEM
    D = pltpu.SemaphoreType.DMA
    wid = 1536
    return pl.pallas_call(
        mixer_kernel,
        name="mixer",
        out_shape=jax.ShapeDtypeStruct((512, wid), BF16),
        in_specs=[pl.BlockSpec(memory_space=V)] * 7,
        out_specs=pl.BlockSpec(memory_space=V),
        scratch_shapes=[
            V((512, wid), BF16), V((512, wid), F32), V((512, wid), F32), V((512, 3072), F32),
            V((24, 512), F32), V((128, wid), F32), V((128, wid), BF16), V((8, 16, wid), BF16),
            V((8, 16, wid), F32), V((8, wid), F32), V((16, wid), BF16), V((8, 16, wid), BF16),
            V((8, 16, wid), BF16), V((128, wid), BF16),
            V((8, 128), F32), V((8, 8, 128), F32), V((8, 128), F32), V((8, 8, 128), F32),
        ] + [D((8,))] * 10,
        compiler_params=pltpu.CompilerParams(
            collective_id=1, has_side_effects=True, vmem_limit_bytes=60 * 2**20),
    )(x, b, c, step.T, ld.T, skip.reshape(1, 24), hg.reshape(1, wid))

def back_kernel(n_ref, res_ref, wo_hbm, wq_hbm, gain_ref, stream_ref, out_ref,
                wo_p, wo_o, wq, base, psend, precv, srecv,
                own, buf, knat, osend, oland,
                w_sem, p_send, p_recv, s_send, s_recv,
                send_sem, recv_sem, hsend_sem, hrecv_sem, osend_sem, orecv_sem):
    z = lax.axis_index("seq_0")
    yh = lax.axis_index("seq_1")
    xx = lax.axis_index("seq_2")
    cc = lax.axis_index("seq_3")
    tp = lax.axis_index("tp")
    g = xx * 2 + cc
    row = z * 2 + yh
    nrow = lax.rem(row + 1, 8)
    prow = lax.rem(row + 7, 8)
    hd, tok, ch, nch, half = 96, 512, 128, 4, 1536

    def at_group(j):
        return {"seq_2": j // 2, "seq_3": lax.rem(j, 2)}

    def at_row(r):
        return {"seq_0": r // 2, "seq_1": lax.rem(r, 2)}

    partner = {"tp": 1 - tp}
    own_cols = pl.ds(pl.multiple_of(tp * half, half), half)
    far_cols = pl.ds(pl.multiple_of((1 - tp) * half, half), half)

    def dot(a, b):
        return jnp.dot(a, b, preferred_element_type=F32)

    loads = [
        pltpu.make_async_copy(wo_hbm.at[:, far_cols], wo_p, w_sem.at[0]),
        pltpu.make_async_copy(wo_hbm.at[:, own_cols], wo_o, w_sem.at[1]),
        pltpu.make_async_copy(wq_hbm, wq, w_sem.at[2]),
    ]
    for load in loads:
        load.start()

    barrier = pltpu.get_barrier_semaphore()
    for d in range(1, 8):
        pl.semaphore_signal(barrier, inc=1, device_id=at_group(lax.rem(g + d, 8)), device_id_type=MESH)
    for dev in (at_row(nrow), at_row(prow), partner):
        pl.semaphore_signal(barrier, inc=1, device_id=dev, device_id_type=MESH)
    pl.semaphore_wait(barrier, 10)

    def rows(c):
        return slice(c * ch, (c + 1) * ch)

    def p_copy(c):
        return pltpu.make_async_remote_copy(
            src_ref=psend.at[c], dst_ref=precv.at[c], send_sem=p_send.at[c],
            recv_sem=p_recv.at[c], device_id=partner, device_id_type=MESH)

    def s_copy(c):
        return pltpu.make_async_remote_copy(
            src_ref=stream_ref.at[pl.ds(c * ch, ch)], dst_ref=srecv.at[c], send_sem=s_send.at[c],
            recv_sem=s_recv.at[c], device_id=partner, device_id_type=MESH)

    loads[0].wait()
    for c in range(nch):
        psend[c] = dot(n_ref[rows(c)], wo_p[...]).astype(BF16)
        p_copy(c).start()
    loads[1].wait()
    for c in range(nch):
        base[rows(c)] = res_ref[rows(c)].astype(F32) + dot(n_ref[rows(c)], wo_o[...])
    for c in range(nch):
        p_copy(c).wait_recv()
        stream_ref[rows(c)] = (base[rows(c)] + precv[c].astype(F32)).astype(BF16)
        s_copy(c).start()
    loads[2].wait()

    def head(j):
        return pl.ds(pl.multiple_of(j * hd, 32), hd)

    def block_copy(c, d):
        j = lax.rem(g + d, 8)
        return pltpu.make_async_remote_copy(
            src_ref=own.at[c, :, head(j), :],
            dst_ref=buf.at[4 + g, c],
            send_sem=send_sem.at[c, d],
            recv_sem=recv_sem.at[c, g],
            device_id=at_group(j), device_id_type=MESH)

    def halo_copy(c, i):
        return pltpu.make_async_remote_copy(
            src_ref=buf.at[8 + i, c, pl.ds(1, 2)],
            dst_ref=buf.at[i, c, pl.ds(1, 2)],
            send_sem=hsend_sem.at[c, i],
            recv_sem=hrecv_sem.at[c, i],
            device_id=at_row(nrow), device_id_type=MESH)

    def out_copy(b):
        return pltpu.make_async_remote_copy(
            src_ref=osend.at[b],
            dst_ref=oland.at[g],
            send_sem=osend_sem.at[b],
            recv_sem=orecv_sem.at[g],
            device_id=at_group(b), device_id_type=MESH)

    def landed(ref, sem):
        pltpu.make_async_copy(ref, ref, sem).wait()

    def arrivals(c):
        for b in (4, 5, 6, 7, 0, 1, 2, 3):
            @pl.when(b != g)
            def _(b=b):
                landed(buf.at[4 + b, c], recv_sem.at[c, b])
            if b >= 4:
                @pl.when(row < 7)
                def _(b=b):
                    halo_copy(c, b - 4).start()
        for b in range(8):
            knat[4 + b, c * ch:(c + 1) * ch, :] = buf[4 + b, c, 1].T

    gain_own = gain_ref[0:1, own_cols]
    gain_far = gain_ref[0:1, far_cols]
    for c in range(nch):
        landed(srecv.at[c], s_recv.at[c])
        a = stream_ref[rows(c)].astype(F32)
        f = srecv[c].astype(F32)
        ss = jnp.sum(a * a, axis=1, keepdims=True) + jnp.sum(f * f, axis=1, keepdims=True)
        inv = lax.rsqrt(ss * (1.0 / (2 * half)) + EPSILON)
        na = (a * inv * gain_own).astype(BF16)
        nf = (f * inv * gain_far).astype(BF16)
        for i in range(3):
            r = dot(na, wq[i, own_cols, :]) + dot(nf, wq[i, far_cols, :])
            own[c, i] = r.astype(BF16).T
        for d in (4, 5, 3, 2, 6, 1, 7):
            block_copy(c, d).start()
        buf[4 + g, c] = own[c, :, head(g), :]
        if c > 0:
            arrivals(c - 1)
    arrivals(nch - 1)

    scale = (hd ** -0.5) * LOG2E
    spos = lax.broadcasted_iota(jnp.int32, (tok, tok), 0)
    tpos = lax.broadcasted_iota(jnp.int32, (tok, tok), 1)
    causal = spos <= tpos

    def wide(j, i):
        return jnp.concatenate([buf[j, c, i] for c in range(nch)], axis=1)

    @pl.when(row == 0)
    def _():
        for i in range(4):
            knat[i] = jnp.zeros((tok, hd), BF16)

    def one_block(step, _):
        b = jnp.where(step < 4, 4 + step, 7 - step)

        @pl.when(jnp.logical_and(step >= 4, row > 0))
        def _():
            for c in range(nch):
                halo_copy(c, b).wait_recv()
                knat[b, c * ch:(c + 1) * ch, :] = buf[b, c, 1].T

        qt = wide(4 + b, 0)
        has_far = jnp.logical_or(step < 4, row > 0)
        s_diag = dot(knat[4 + b], qt)
        s_far = dot(knat[b], qt)
        s = jnp.where(causal, s_diag, jnp.where(has_far, s_far, NEG))
        m = jnp.max(s, axis=0, keepdims=True)
        p = jnp.exp2((s - m) * scale)
        l = jnp.sum(p, axis=0, keepdims=True)
        p_diag = jnp.where(causal, p, 0.0).astype(BF16)
        acc = dot(wide(4 + b, 2), p_diag)
        p_far = jnp.where(causal, 0.0, p).astype(BF16)
        v_far = jnp.where(has_far, wide(b, 2), jnp.zeros((hd, tok), BF16))
        acc = acc + dot(v_far, p_far)

        def mid(j, carry):
            m, l, acc = carry
            s = dot(knat[j], qt)
            m_new = jnp.maximum(m, jnp.max(s, axis=0, keepdims=True))
            alpha = jnp.exp2((m - m_new) * scale)
            p = jnp.exp2((s - m_new) * scale)
            l = alpha * l + jnp.sum(p, axis=0, keepdims=True)
            acc = alpha * acc + dot(wide(j, 2), p.astype(BF16))
            return m_new, l, acc

        first = jnp.where(row > 0, b + 1, jnp.maximum(b + 1, 4))
        m, l, acc = lax.fori_loop(first, b + 4, mid, (m, l, acc))
        osend[b] = (acc / l).astype(BF16)

        @pl.when(b != g)
        def _():
            out_copy(b).start()
        return 0

    lax.fori_loop(0, 8, one_block, 0)
    oland[g] = osend[g]
    for b in range(8):
        @pl.when(b != g)
        def _(b=b):
            landed(oland.at[b], orecv_sem.at[b])
    out_ref[...] = oland[...].reshape(8 * hd, tok).T
    for c in range(nch):
        p_copy(c).wait_send()
        s_copy(c).wait_send()
        for d in range(1, 8):
            block_copy(c, d).wait_send()
    for b in range(8):
        @pl.when(b != g)
        def _(b=b):
            out_copy(b).wait_send()

    @pl.when(row < 7)
    def _():
        for c in range(nch):
            for i in range(4):
                halo_copy(c, i).wait_send()


def back(normed, residual, mixer_out, weight, gain):
    V = pltpu.VMEM
    D = pltpu.SemaphoreType.DMA
    vm = pl.BlockSpec(memory_space=V)
    hbm = pl.BlockSpec(memory_space=pl.ANY)
    return pl.pallas_call(
        back_kernel,
        name="back",
        out_shape=(jax.ShapeDtypeStruct((512, 1536), BF16), jax.ShapeDtypeStruct((512, 768), BF16)),
        in_specs=[vm, vm, hbm, hbm, vm],
        out_specs=(vm, vm),
        scratch_shapes=[
            V((1536, 1536), BF16), V((1536, 1536), BF16), V((3, 3072, 768), BF16),
            V((512, 1536), F32), V((4, 128, 1536), BF16), V((4, 128, 1536), BF16), V((4, 128, 1536), BF16),
            V((4, 3, 768, 128), BF16), V((12, 4, 3, 96, 128), BF16), V((12, 512, 96), BF16),
            V((8, 96, 512), BF16), V((8, 96, 512), BF16),
            D((3,)), D((4,)), D((4,)), D((4,)), D((4,)),
            D((4, 8)), D((4, 8)), D((4, 4)), D((4, 4)), D((8,)), D((8,)),
        ],
        compiler_params=pltpu.CompilerParams(
            collective_id=2, has_side_effects=True, vmem_limit_bytes=63 * 2**20),
    )(normed, residual, mixer_out, weight, gain.reshape(1, 3072))


def on_device(
    mixer_input,
    state_write,
    state_read,
    step_size,
    log_decay,
    skip_gain,
    head_gain,
    mixer_out,
    residual,
    attn_gain,
    qkv_weight,
):
    normed = mixer(mixer_input, state_write, state_read, step_size, log_decay, skip_gain, head_gain)
    weight = jnp.transpose(qkv_weight, (1, 0, 2))
    stream, pieces = back(normed, residual, mixer_out, weight, attn_gain)
    return (stream, pieces)


def solution(mesh):
    torus = Mesh(
        mesh.devices.reshape(4, 2, 4, 2, mesh.shape["tp"]),
        ("seq_0", "seq_1", "seq_2", "seq_3", "tp"),
    )
    in_specs = (
        P(SEQ, "tp"),
        P(SEQ, None),
        P(SEQ, None),
        P(SEQ, "tp"),
        P(SEQ, "tp"),
        P("tp"),
        P("tp"),
        P("tp", None),
        P(SEQ, "tp"),
        P(),
        P(None, None, "tp"),
    )
    out_specs = (P(SEQ, "tp"), P(SEQ, "tp"))
    return jax.shard_map(
        on_device, mesh=torus, in_specs=in_specs, out_specs=out_specs, check_vma=False
    )
```

```python
import jax
import jax.numpy as jnp
from jax import lax
from jax.sharding import Mesh
from jax.experimental import pallas as pl
from jax.experimental.pallas import tpu as pltpu
from jax.sharding import PartitionSpec as P

SEQ = ("seq_0", "seq_1", "seq_2", "seq_3")


EPSILON = 1e-05


MESH = pl.DeviceIdType.MESH
F32 = jnp.float32
BF16 = jnp.bfloat16
NEG = -1e30
LOG2E = 1.4426950408889634


def parts_of(v, count):
    out = []
    for _ in range(count):
        piece = v.astype(BF16)
        out.append(piece)
        v = v - piece.astype(F32)
    return out


def one_hot(shape, per_lane, period=None):
    r = lax.broadcasted_iota(jnp.int32, shape, 0)
    c = lax.broadcasted_iota(jnp.int32, shape, 1)
    if period is not None:
        r = lax.rem(r, period)
    return jnp.where(r == c // per_lane, 1.0, 0.0).astype(BF16)


def mixer_kernel(x_ref, b_ref, c_ref, step_ref, ld_ref, skip_ref, hg_ref, n_ref,
                 u, ybuf, eexp, gexp, gt, s0, stage, rs, pref, dpre, rowst, rr, back, cin,
                 tst, tr, rtst, rtr,
                 a_send, a_recv, at_send, at_recv, r_send, r_recv, rt_send, rt_recv,
                 c_send, c_recv):
    z = lax.axis_index("seq_0")
    yh = lax.axis_index("seq_1")
    xx = lax.axis_index("seq_2")
    cc = lax.axis_index("seq_3")
    g = xx * 2 + cc
    row = z * 2 + yh
    nh, blk, wid = 24, 256, 1536

    def at_group(j):
        return {"seq_2": j // 2, "seq_3": lax.rem(j, 2)}

    def at_row(r):
        return {"seq_0": r // 2, "seq_1": lax.rem(r, 2)}

    barrier = pltpu.get_barrier_semaphore()
    for d in range(1, 8):
        pl.semaphore_signal(barrier, inc=1, device_id=at_group(lax.rem(g + d, 8)), device_id_type=MESH)
        pl.semaphore_signal(barrier, inc=1, device_id=at_row(lax.rem(row + d, 8)), device_id_type=MESH)

    def dot(a, b):
        return jnp.dot(a, b, preferred_element_type=F32)

    si = lax.broadcasted_iota(jnp.int32, (blk, blk), 0)
    ti = lax.broadcasted_iota(jnp.int32, (blk, blk), 1)
    upto = jnp.where(si <= ti, 1.0, 0.0).astype(BF16)
    wt = []
    for c in range(2):
        ld = ld_ref[:, c * blk:(c + 1) * blk]
        cat = jnp.concatenate(parts_of(ld, 3), axis=0)
        r = dot(cat, upto)
        gtc = (r[0:nh] + r[nh:2 * nh] + r[2 * nh:3 * nh]) * LOG2E
        gt[:, c * blk:(c + 1) * blk] = gtc
        wt.append(jnp.exp2(gtc[:, blk - 1:blk] - gtc))
    gtv = gt[...]
    g_col = gtv.T
    total = g_col[blk - 1:blk] + g_col[2 * blk - 1:2 * blk]
    tst[...] = jnp.zeros((8, 128), F32)
    tst[0:1, 0:nh] = total

    e3 = one_hot((3 * nh, wid), 64, nh)

    def expand(v, count=3):
        k = count * nh
        return dot(jnp.concatenate(parts_of(v, count), axis=1), e3[0:k] if count < 3 else e3)

    step_col = step_ref[...].T
    w_col = jnp.concatenate(wt, axis=1).T
    e_col = jnp.exp2(g_col)
    state = None
    for c in range(2):
        rows = slice(c * blk, (c + 1) * blk)
        uc = (expand(step_col[rows]) * x_ref[rows].astype(F32)).astype(BF16)
        u[rows] = uc
        wu = (expand(w_col[rows]) * uc.astype(F32)).astype(BF16)
        term = dot(b_ref[rows].T, wu)
        if c == 0:
            s0[...] = term
        else:
            state = expand(e_col[2 * blk - 8:2 * blk])[7:8] * s0[...] + term
    stage[...] = state.astype(BF16)
    pl.semaphore_wait(barrier, 14)

    def slice_of(j):
        return pl.ds(pl.multiple_of(j * 16, 16), 16)

    def a_copy(d):
        j = lax.rem(g + d, 8)
        return pltpu.make_async_remote_copy(
            src_ref=stage.at[slice_of(j)], dst_ref=rs.at[g],
            send_sem=a_send.at[d], recv_sem=a_recv.at[g],
            device_id=at_group(j), device_id_type=MESH)

    def at_copy(d):
        j = lax.rem(g + d, 8)
        return pltpu.make_async_remote_copy(
            src_ref=tst, dst_ref=tr.at[g],
            send_sem=at_send.at[d], recv_sem=at_recv.at[g],
            device_id=at_group(j), device_id_type=MESH)

    def r_copy(d):
        return pltpu.make_async_remote_copy(
            src_ref=rowst, dst_ref=rr.at[row],
            send_sem=r_send.at[d], recv_sem=r_recv.at[row],
            device_id=at_row(lax.rem(row + d, 8)), device_id_type=MESH)

    def rt_copy(d):
        return pltpu.make_async_remote_copy(
            src_ref=rtst, dst_ref=rtr.at[row],
            send_sem=rt_send.at[d], recv_sem=rt_recv.at[row],
            device_id=at_row(lax.rem(row + d, 8)), device_id_type=MESH)

    def c_copy(j):
        return pltpu.make_async_remote_copy(
            src_ref=back.at[j], dst_ref=cin.at[slice_of(g)],
            send_sem=c_send.at[j], recv_sem=c_recv.at[g],
            device_id=at_group(j), device_id_type=MESH)

    def landed(ref, sem):
        pltpu.make_async_copy(ref, ref, sem).wait()

    for d in range(1, 8):
        at_copy(d).start()
    for d in (4, 5, 3, 2, 6, 1, 7):
        a_copy(d).start()
    rs[g] = stage[slice_of(g), :]
    tr[g] = tst[...]
    one3 = one_hot((3 * nh, nh * 128), 128, nh)
    gexp[...] = dot(jnp.concatenate(parts_of(g_col, 3), axis=1), one3)
    eexp[...] = expand(e_col)

    causal = si >= ti

    def local_pairs(c, lo, hi):
        rows = slice(c * blk, (c + 1) * blk)
        cb = lax.dot_general(c_ref[rows], b_ref[rows], (((1,), (1,)), ((), ())),
                             preferred_element_type=F32)
        cb = jnp.where(causal, cb, 0.0)
        lane = lax.broadcasted_iota(jnp.int32, (blk, 128), 1)

        def pair(p, _):
            off = pl.multiple_of(p * 128, 128)
            up = u[rows, pl.ds(off, 128)]
            ys = []
            for k in range(2):
                h = p * 2 + k
                gc = gexp[rows, pl.ds(pl.multiple_of(h * 128, 128), 128)]
                gr = gt[pl.ds(h, 1), rows]
                gap = jnp.concatenate([gc, gc], axis=1) - gr
                m = (jnp.exp2(jnp.minimum(gap, 0.0)) * cb).astype(BF16)
                ys.append(dot(m, up))
            ybuf[rows, pl.ds(off, 128)] = jnp.where(lane < 64, ys[0], ys[1])
            return 0

        lax.fori_loop(lo, hi, pair, 0)

    local_pairs(0, 0, 12)

    for j in range(8):
        @pl.when(j != g)
        def _(j=j):
            landed(tr.at[j], at_recv.at[j])
            landed(rs.at[j], a_recv.at[j])
    e128 = one_hot((128, wid), 64)

    def table(ref):
        t = jnp.concatenate([ref[j, 0:1, :] for j in range(8)], axis=0)
        return t

    def spread(t):
        p = parts_of(t, 3)
        return dot(p[0], e128) + dot(p[1], e128) + dot(p[2], e128)

    tt = table(tr)
    dec = spread(jnp.exp2(tt))
    run = jnp.zeros((16, wid), F32)
    dr = jnp.ones((1, wid), F32)
    for j in range(8):
        pref[j] = run
        dpre[j:j + 1] = dr
        run = run * dec[j:j + 1] + rs[j].astype(F32)
        dr = dr * dec[j:j + 1]
    rowst[...] = run.astype(BF16)
    rtst[...] = jnp.broadcast_to(jnp.sum(tt, axis=0, keepdims=True), (8, 128))
    for d in range(1, 8):
        @pl.when(row + d < 8)
        def _(d=d):
            rt_copy(d).start()
            r_copy(d).start()

    local_pairs(1, 0, 8)

    for r in range(7):
        @pl.when(r < row)
        def _(r=r):
            landed(rtr.at[r], rt_recv.at[r])
            landed(rr.at[r], r_recv.at[r])
    rmask = lax.broadcasted_iota(jnp.int32, (8, 128), 0) < row
    rdec = spread(jnp.where(rmask, jnp.exp2(table(rtr)), 0.0))
    rc = jnp.zeros((16, wid), F32)
    for r in range(7):
        rc = jnp.where(r < row, rc * rdec[r:r + 1] + rr[r].astype(F32), rc)
    for j in range(8):
        back[j] = (pref[j] + dpre[j:j + 1] * rc).astype(BF16)
    for d in (4, 5, 3, 2, 6, 1, 7):
        c_copy(lax.rem(g + d, 8)).start()
    cin[slice_of(g), :] = back[g]

    local_pairs(1, 8, 12)

    skip = expand(jnp.broadcast_to(skip_ref[...], (8, nh)))[0:1]
    et = jnp.where(lax.broadcasted_iota(jnp.int32, (wid, nh), 0) // 64
                   == lax.broadcasted_iota(jnp.int32, (wid, nh), 1), 1.0, 0.0).astype(BF16)
    for j in range(8):
        @pl.when(j != g)
        def _(j=j):
            landed(cin.at[pl.ds(j * 16, 16)], c_recv.at[j])
    entering = cin[...].astype(F32)
    for c in range(2):
        rows = slice(c * blk, (c + 1) * blk)
        if c == 1:
            entering = eexp[blk - 1:blk] * entering + s0[...]
        y = ybuf[rows] + eexp[rows] * dot(c_ref[rows], entering.astype(BF16))
        y = y + skip * x_ref[rows].astype(F32)
        sq = parts_of(y * y, 2)
        ssum = dot(sq[0], et) + dot(sq[1], et)
        inv = lax.rsqrt(ssum * (1.0 / 64.0) + EPSILON)
        n_ref[rows] = (y * expand(inv) * hg_ref[...].reshape(1, wid)).astype(BF16)

    for d in range(1, 8):
        at_copy(d).wait_send()
        a_copy(d).wait_send()
        c_copy(lax.rem(g + d, 8)).wait_send()

        @pl.when(row + d < 8)
        def _(d=d):
            rt_copy(d).wait_send()
            r_copy(d).wait_send()


def mixer(x, b, c, step, ld, skip, hg):
    V = pltpu.VMEM
    D = pltpu.SemaphoreType.DMA
    wid = 1536
    return pl.pallas_call(
        mixer_kernel,
        name="mixer",
        out_shape=jax.ShapeDtypeStruct((512, wid), BF16),
        in_specs=[pl.BlockSpec(memory_space=V)] * 7,
        out_specs=pl.BlockSpec(memory_space=V),
        scratch_shapes=[
            V((512, wid), BF16), V((512, wid), F32), V((512, wid), F32), V((512, 3072), F32),
            V((24, 512), F32), V((128, wid), F32), V((128, wid), BF16), V((8, 16, wid), BF16),
            V((8, 16, wid), F32), V((8, wid), F32), V((16, wid), BF16), V((8, 16, wid), BF16),
            V((8, 16, wid), BF16), V((128, wid), BF16),
            V((8, 128), F32), V((8, 8, 128), F32), V((8, 128), F32), V((8, 8, 128), F32),
        ] + [D((8,))] * 10,
        compiler_params=pltpu.CompilerParams(
            collective_id=1, has_side_effects=True, vmem_limit_bytes=60 * 2**20),
    )(x, b, c, step.T, ld.T, skip.reshape(1, 24), hg)

def back_kernel(n_ref, res_ref, wo_hbm, wq_hbm, gain_ref, stream_ref, out_ref,
                wo_p, wo_o, wq, base, psend, precv, srecv,
                own, buf, knat, osend, oland, mkeep, lkeep, akeep,
                w_sem, p_send, p_recv, s_send, s_recv,
                send_sem, recv_sem, hsend_sem, hrecv_sem, osend_sem, orecv_sem):
    z = lax.axis_index("seq_0")
    yh = lax.axis_index("seq_1")
    xx = lax.axis_index("seq_2")
    cc = lax.axis_index("seq_3")
    tp = lax.axis_index("tp")
    g = xx * 2 + cc
    row = z * 2 + yh
    nrow = lax.rem(row + 1, 8)
    prow = lax.rem(row + 7, 8)
    hd, tok, ch, nch, half = 96, 512, 128, 4, 1536

    def at_group(j):
        return {"seq_2": j // 2, "seq_3": lax.rem(j, 2)}

    def at_row(r):
        return {"seq_0": r // 2, "seq_1": lax.rem(r, 2)}

    partner = {"tp": 1 - tp}
    own_cols = pl.ds(pl.multiple_of(tp * half, half), half)
    far_cols = pl.ds(pl.multiple_of((1 - tp) * half, half), half)

    def dot(a, b):
        return jnp.dot(a, b, preferred_element_type=F32)

    loads = [
        pltpu.make_async_copy(wo_hbm.at[:, far_cols], wo_p, w_sem.at[0]),
        pltpu.make_async_copy(wo_hbm.at[:, own_cols], wo_o, w_sem.at[1]),
        pltpu.make_async_copy(wq_hbm, wq, w_sem.at[2]),
    ]
    for load in loads:
        load.start()

    barrier = pltpu.get_barrier_semaphore()
    for d in range(1, 8):
        pl.semaphore_signal(barrier, inc=1, device_id=at_group(lax.rem(g + d, 8)), device_id_type=MESH)
    for dev in (at_row(nrow), at_row(prow), partner):
        pl.semaphore_signal(barrier, inc=1, device_id=dev, device_id_type=MESH)
    pl.semaphore_wait(barrier, 10)

    def rows(c):
        return slice(c * ch, (c + 1) * ch)

    def p_copy(c):
        return pltpu.make_async_remote_copy(
            src_ref=psend.at[c], dst_ref=precv.at[c], send_sem=p_send.at[c],
            recv_sem=p_recv.at[c], device_id=partner, device_id_type=MESH)

    def s_copy(c):
        return pltpu.make_async_remote_copy(
            src_ref=stream_ref.at[pl.ds(c * ch, ch)], dst_ref=srecv.at[c], send_sem=s_send.at[c],
            recv_sem=s_recv.at[c], device_id=partner, device_id_type=MESH)

    loads[0].wait()
    for c in range(nch):
        psend[c] = dot(n_ref[rows(c)], wo_p[...]).astype(BF16)
        p_copy(c).start()
    loads[1].wait()
    for c in range(nch):
        base[rows(c)] = res_ref[rows(c)].astype(F32) + dot(n_ref[rows(c)], wo_o[...])
    for c in range(nch):
        p_copy(c).wait_recv()
        stream_ref[rows(c)] = (base[rows(c)] + precv[c].astype(F32)).astype(BF16)
        s_copy(c).start()
    loads[2].wait()

    def head(j):
        return pl.ds(pl.multiple_of(j * hd, 32), hd)

    def block_copy(c, d):
        j = lax.rem(g + d, 8)
        return pltpu.make_async_remote_copy(
            src_ref=own.at[c, :, head(j), :],
            dst_ref=buf.at[4 + g, c],
            send_sem=send_sem.at[c, d],
            recv_sem=recv_sem.at[c, g],
            device_id=at_group(j), device_id_type=MESH)

    def halo_copy(c, i):
        return pltpu.make_async_remote_copy(
            src_ref=buf.at[8 + i, c, pl.ds(1, 2)],
            dst_ref=buf.at[i, c, pl.ds(1, 2)],
            send_sem=hsend_sem.at[c, i],
            recv_sem=hrecv_sem.at[c, i],
            device_id=at_row(nrow), device_id_type=MESH)

    def out_copy(b):
        return pltpu.make_async_remote_copy(
            src_ref=osend.at[b],
            dst_ref=oland.at[g],
            send_sem=osend_sem.at[b],
            recv_sem=orecv_sem.at[g],
            device_id=at_group(b), device_id_type=MESH)

    def landed(ref, sem):
        pltpu.make_async_copy(ref, ref, sem).wait()

    def arrivals(c):
        for b in (4, 5, 6, 7, 0, 1, 2, 3):
            @pl.when(b != g)
            def _(b=b):
                landed(buf.at[4 + b, c], recv_sem.at[c, b])
            if b >= 4:
                @pl.when(row < 7)
                def _(b=b):
                    halo_copy(c, b - 4).start()
        for b in range(8):
            knat[4 + b, c * ch:(c + 1) * ch, :] = buf[4 + b, c, 1].T

    gain_own = gain_ref[own_cols].reshape(1, half)
    gain_far = gain_ref[far_cols].reshape(1, half)
    for c in range(nch):
        landed(srecv.at[c], s_recv.at[c])
        a = stream_ref[rows(c)].astype(F32)
        f = srecv[c].astype(F32)
        ss = jnp.sum(a * a, axis=1, keepdims=True) + jnp.sum(f * f, axis=1, keepdims=True)
        inv = lax.rsqrt(ss * (1.0 / (2 * half)) + EPSILON)
        na = (a * inv * gain_own).astype(BF16)
        nf = (f * inv * gain_far).astype(BF16)
        for i in range(3):
            r = dot(na, wq[i, own_cols, :]) + dot(nf, wq[i, far_cols, :])
            own[c, i] = r.astype(BF16).T
        for d in (4, 5, 3, 2, 6, 1, 7):
            block_copy(c, d).start()
        buf[4 + g, c] = own[c, :, head(g), :]
        if c > 0:
            arrivals(c - 1)
    scale = (hd ** -0.5) * LOG2E
    early = 3 * ch

    def causal(n):
        return (lax.broadcasted_iota(jnp.int32, (n, n), 0)
                <= lax.broadcasted_iota(jnp.int32, (n, n), 1))

    def wide(j, i, lo, hi):
        return jnp.concatenate([buf[j, c, i] for c in range(lo, hi)], axis=1)

    @pl.when(row == 0)
    def _():
        for i in range(4):
            knat[i] = jnp.zeros((tok, hd), BF16)
            for c in range(nch):
                buf[i, c, 2] = jnp.zeros((hd, ch), BF16)

    def order(step):
        return jnp.where(step < 4, 4 + step, 7 - step)

    def halo_in(step, b, lo, hi):
        @pl.when(jnp.logical_and(step >= 4, row > 0))
        def _():
            for c in range(lo, hi):
                halo_copy(c, b).wait_recv()
                knat[b, c * ch:(c + 1) * ch, :] = buf[b, c, 1].T

    low = causal(early)

    def first_round(step, _):
        b = order(step)
        halo_in(step, b, 0, 3)
        qt = wide(4 + b, 0, 0, 3)
        has_far = jnp.logical_or(step < 4, row > 0)
        s_diag = dot(knat[4 + b, 0:early], qt)
        s_far = dot(knat[b, 0:early], qt)
        s = jnp.where(low, s_diag, jnp.where(has_far, s_far, NEG))
        m = jnp.max(s, axis=0, keepdims=True)
        p = jnp.exp2((s - m) * scale)
        l = jnp.sum(p, axis=0, keepdims=True)
        acc = dot(wide(4 + b, 2, 0, 3), jnp.where(low, p, 0.0).astype(BF16))
        acc = acc + dot(wide(b, 2, 0, 3), jnp.where(low, 0.0, p).astype(BF16))

        def mid(j, carry):
            m, l, acc = carry
            s = dot(knat[j, 0:early], qt)
            m_new = jnp.maximum(m, jnp.max(s, axis=0, keepdims=True))
            alpha = jnp.exp2((m - m_new) * scale)
            p = jnp.exp2((s - m_new) * scale)
            l = alpha * l + jnp.sum(p, axis=0, keepdims=True)
            acc = alpha * acc + dot(wide(j, 2, 0, 3), p.astype(BF16))
            return m_new, l, acc

        first = jnp.where(row > 0, b + 1, jnp.maximum(b + 1, 4))
        m, l, acc = lax.fori_loop(first, b + 4, mid, (m, l, acc))
        mkeep[b] = m
        lkeep[b] = l
        akeep[b] = acc
        return 0

    lax.fori_loop(0, 8, first_round, 0)
    arrivals(nch - 1)
    low1 = causal(ch)

    def second_round(step, _):
        b = order(step)
        halo_in(step, b, 3, 4)

        def there(i):
            return jnp.logical_or(b + i >= 4, row > 0)

        qt = wide(4 + b, 0, 0, 3)
        ss = [jnp.where(there(i), dot(knat[b + i, early:tok], qt), NEG) for i in range(4)]
        m = mkeep[b]
        m_new = m
        for t in ss:
            m_new = jnp.maximum(m_new, jnp.max(t, axis=0, keepdims=True))
        alpha = jnp.exp2((m - m_new) * scale)
        ps = [jnp.exp2((t - m_new) * scale) for t in ss]
        l = alpha * lkeep[b]
        for t in ps:
            l = l + jnp.sum(t, axis=0, keepdims=True)
        pt = jnp.concatenate([t.astype(BF16) for t in ps], axis=0)
        vt = jnp.concatenate([buf[b + i, 3, 2] for i in range(4)], axis=1)
        acc = alpha * akeep[b] + dot(vt, pt)
        osend[b, :, 0:early] = (acc / l).astype(BF16)

        qt = buf[4 + b, 3, 0]
        s_diag = dot(knat[4 + b, early:tok], qt)
        s_far = dot(knat[b, early:tok], qt)
        ss = [jnp.where(low1, s_diag, jnp.where(there(0), s_far, NEG)), dot(knat[4 + b, 0:early], qt)]
        ss += [jnp.where(there(i), dot(knat[b + i], qt), NEG) for i in range(1, 4)]
        m = jnp.max(ss[0], axis=0, keepdims=True)
        for t in ss[1:]:
            m = jnp.maximum(m, jnp.max(t, axis=0, keepdims=True))
        ps = [jnp.exp2((t - m) * scale) for t in ss]
        l = jnp.sum(ps[0], axis=0, keepdims=True)
        for t in ps[1:]:
            l = l + jnp.sum(t, axis=0, keepdims=True)
        pt = jnp.concatenate(
            [jnp.where(low1, ps[0], 0.0).astype(BF16), jnp.where(low1, 0.0, ps[0]).astype(BF16)]
            + [t.astype(BF16) for t in ps[1:]], axis=0)
        vt = jnp.concatenate(
            [buf[4 + b, 3, 2], buf[b, 3, 2], wide(4 + b, 2, 0, 3)]
            + [wide(b + i, 2, 0, 4) for i in range(1, 4)], axis=1)
        osend[b, :, early:tok] = (dot(vt, pt) / l).astype(BF16)

        @pl.when(b != g)
        def _():
            out_copy(b).start()
        return 0

    lax.fori_loop(0, 8, second_round, 0)
    oland[g] = osend[g]
    for b in range(8):
        @pl.when(b != g)
        def _(b=b):
            landed(oland.at[b], orecv_sem.at[b])
    out_ref[...] = oland[...].reshape(8 * hd, tok).T
    for c in range(nch):
        p_copy(c).wait_send()
        s_copy(c).wait_send()
        for d in range(1, 8):
            block_copy(c, d).wait_send()
    for b in range(8):
        @pl.when(b != g)
        def _(b=b):
            out_copy(b).wait_send()

    @pl.when(row < 7)
    def _():
        for c in range(nch):
            for i in range(4):
                halo_copy(c, i).wait_send()


def back(normed, residual, mixer_out, weight, gain):
    V = pltpu.VMEM
    D = pltpu.SemaphoreType.DMA
    vm = pl.BlockSpec(memory_space=V)
    hbm = pl.BlockSpec(memory_space=pl.ANY)
    return pl.pallas_call(
        back_kernel,
        name="back",
        out_shape=(jax.ShapeDtypeStruct((512, 1536), BF16), jax.ShapeDtypeStruct((512, 768), BF16)),
        in_specs=[vm, vm, hbm, hbm, vm],
        out_specs=(vm, vm),
        scratch_shapes=[
            V((1536, 1536), BF16), V((1536, 1536), BF16), V((3, 3072, 768), BF16),
            V((512, 1536), F32), V((4, 128, 1536), BF16), V((4, 128, 1536), BF16), V((4, 128, 1536), BF16),
            V((4, 3, 768, 128), BF16), V((12, 4, 3, 96, 128), BF16), V((12, 512, 96), BF16),
            V((8, 96, 512), BF16), V((8, 96, 512), BF16),
            V((8, 1, 384), F32), V((8, 1, 384), F32), V((8, 96, 384), F32),
            D((3,)), D((4,)), D((4,)), D((4,)), D((4,)),
            D((4, 8)), D((4, 8)), D((4, 4)), D((4, 4)), D((8,)), D((8,)),
        ],
        compiler_params=pltpu.CompilerParams(
            collective_id=2, has_side_effects=True, vmem_limit_bytes=63 * 2**20),
    )(normed, residual, mixer_out, weight, gain)


def on_device(
    mixer_input,
    state_write,
    state_read,
    step_size,
    log_decay,
    skip_gain,
    head_gain,
    mixer_out,
    residual,
    attn_gain,
    qkv_weight,
):
    normed = mixer(mixer_input, state_write, state_read, step_size, log_decay, skip_gain, head_gain)
    weight = jnp.transpose(qkv_weight, (1, 0, 2))
    stream, pieces = back(normed, residual, mixer_out, weight, attn_gain)
    return (stream, pieces)


def solution(mesh):
    torus = Mesh(
        mesh.devices.reshape(4, 2, 4, 2, mesh.shape["tp"]),
        ("seq_0", "seq_1", "seq_2", "seq_3", "tp"),
    )
    in_specs = (
        P(SEQ, "tp"),
        P(SEQ, None),
        P(SEQ, None),
        P(SEQ, "tp"),
        P(SEQ, "tp"),
        P("tp"),
        P("tp"),
        P("tp", None),
        P(SEQ, "tp"),
        P(),
        P(None, None, "tp"),
    )
    out_specs = (P(SEQ, "tp"), P(SEQ, "tp"))
    return jax.shard_map(
        on_device, mesh=torus, in_specs=in_specs, out_specs=out_specs, check_vma=False
    )
```

```python
import jax
import jax.numpy as jnp
from jax import lax
from jax.sharding import Mesh
from jax.experimental import pallas as pl
from jax.experimental.pallas import tpu as pltpu
from jax.sharding import PartitionSpec as P

SEQ = ("seq_0", "seq_1", "seq_2", "seq_3")


EPSILON = 1e-05


MESH = pl.DeviceIdType.MESH
F32 = jnp.float32
BF16 = jnp.bfloat16
NEG = -1e30
LOG2E = 1.4426950408889634


def parts_of(v, count):
    out = []
    for _ in range(count):
        piece = v.astype(BF16)
        out.append(piece)
        v = v - piece.astype(F32)
    return out


def one_hot(shape, per_lane, period=None):
    r = lax.broadcasted_iota(jnp.int32, shape, 0)
    c = lax.broadcasted_iota(jnp.int32, shape, 1)
    if period is not None:
        r = lax.rem(r, period)
    return jnp.where(r == c // per_lane, 1.0, 0.0).astype(BF16)


def mixer_kernel(x_ref, b_ref, c_ref, step_ref, ld_ref, skip_ref, hg_ref, n_ref,
                 u, ybuf, eexp, gexp, gt, s0, stage, rs, pref, dpre, rowst, rr, back, cin,
                 tst, tr, rtst, rtr,
                 a_send, a_recv, at_send, at_recv, r_send, r_recv, rt_send, rt_recv,
                 c_send, c_recv):
    z = lax.axis_index("seq_0")
    yh = lax.axis_index("seq_1")
    xx = lax.axis_index("seq_2")
    cc = lax.axis_index("seq_3")
    g = xx * 2 + cc
    row = z * 2 + yh
    nh, blk, wid = 24, 256, 1536

    def at_group(j):
        return {"seq_2": j // 2, "seq_3": lax.rem(j, 2)}

    def at_row(r):
        return {"seq_0": r // 2, "seq_1": lax.rem(r, 2)}

    barrier = pltpu.get_barrier_semaphore()
    for d in range(1, 8):
        pl.semaphore_signal(barrier, inc=1, device_id=at_group(lax.rem(g + d, 8)), device_id_type=MESH)
        pl.semaphore_signal(barrier, inc=1, device_id=at_row(lax.rem(row + d, 8)), device_id_type=MESH)

    def dot(a, b):
        return jnp.dot(a, b, preferred_element_type=F32)

    si = lax.broadcasted_iota(jnp.int32, (blk, blk), 0)
    ti = lax.broadcasted_iota(jnp.int32, (blk, blk), 1)
    upto = jnp.where(si <= ti, 1.0, 0.0).astype(BF16)
    wt = []
    for c in range(2):
        ld = ld_ref[:, c * blk:(c + 1) * blk]
        cat = jnp.concatenate(parts_of(ld, 3), axis=0)
        r = dot(cat, upto)
        gtc = (r[0:nh] + r[nh:2 * nh] + r[2 * nh:3 * nh]) * LOG2E
        gt[:, c * blk:(c + 1) * blk] = gtc
        wt.append(jnp.exp2(gtc[:, blk - 1:blk] - gtc))
    gtv = gt[...]
    g_col = gtv.T
    total = g_col[blk - 1:blk] + g_col[2 * blk - 1:2 * blk]
    tst[...] = jnp.zeros((8, 128), F32)
    tst[0:1, 0:nh] = total

    e3 = one_hot((3 * nh, wid), 64, nh)

    def expand(v, count=3):
        k = count * nh
        return dot(jnp.concatenate(parts_of(v, count), axis=1), e3[0:k] if count < 3 else e3)

    step_col = step_ref[...].T
    w_col = jnp.concatenate(wt, axis=1).T
    e_col = jnp.exp2(g_col)
    state = None
    for c in range(2):
        rows = slice(c * blk, (c + 1) * blk)
        uc = (expand(step_col[rows]) * x_ref[rows].astype(F32)).astype(BF16)
        u[rows] = uc
        wu = (expand(w_col[rows]) * uc.astype(F32)).astype(BF16)
        term = dot(b_ref[rows].T, wu)
        if c == 0:
            s0[...] = term
        else:
            state = expand(e_col[2 * blk - 8:2 * blk])[7:8] * s0[...] + term
    stage[...] = state.astype(BF16)
    pl.semaphore_wait(barrier, 14)

    def slice_of(j):
        return pl.ds(pl.multiple_of(j * 16, 16), 16)

    def a_copy(d):
        j = lax.rem(g + d, 8)
        return pltpu.make_async_remote_copy(
            src_ref=stage.at[slice_of(j)], dst_ref=rs.at[g],
            send_sem=a_send.at[d], recv_sem=a_recv.at[g],
            device_id=at_group(j), device_id_type=MESH)

    def at_copy(d):
        j = lax.rem(g + d, 8)
        return pltpu.make_async_remote_copy(
            src_ref=tst, dst_ref=tr.at[g],
            send_sem=at_send.at[d], recv_sem=at_recv.at[g],
            device_id=at_group(j), device_id_type=MESH)

    def r_copy(d):
        return pltpu.make_async_remote_copy(
            src_ref=rowst, dst_ref=rr.at[row],
            send_sem=r_send.at[d], recv_sem=r_recv.at[row],
            device_id=at_row(lax.rem(row + d, 8)), device_id_type=MESH)

    def rt_copy(d):
        return pltpu.make_async_remote_copy(
            src_ref=rtst, dst_ref=rtr.at[row],
            send_sem=rt_send.at[d], recv_sem=rt_recv.at[row],
            device_id=at_row(lax.rem(row + d, 8)), device_id_type=MESH)

    def c_copy(j):
        return pltpu.make_async_remote_copy(
            src_ref=back.at[j], dst_ref=cin.at[slice_of(g)],
            send_sem=c_send.at[j], recv_sem=c_recv.at[g],
            device_id=at_group(j), device_id_type=MESH)

    def landed(ref, sem):
        pltpu.make_async_copy(ref, ref, sem).wait()

    for d in range(1, 8):
        at_copy(d).start()
    for d in (4, 5, 3, 2, 6, 1, 7):
        a_copy(d).start()
    rs[g] = stage[slice_of(g), :]
    tr[g] = tst[...]
    one3 = one_hot((3 * nh, nh * 128), 128, nh)
    gexp[...] = dot(jnp.concatenate(parts_of(g_col, 3), axis=1), one3)
    eexp[...] = expand(e_col)

    causal = si >= ti

    def local_pairs(c, lo, hi):
        rows = slice(c * blk, (c + 1) * blk)
        cb = lax.dot_general(c_ref[rows], b_ref[rows], (((1,), (1,)), ((), ())),
                             preferred_element_type=F32)
        cb = jnp.where(causal, cb, 0.0)
        lane = lax.broadcasted_iota(jnp.int32, (blk, 128), 1)

        def pair(p, _):
            off = pl.multiple_of(p * 128, 128)
            up = u[rows, pl.ds(off, 128)]
            ys = []
            for k in range(2):
                h = p * 2 + k
                gc = gexp[rows, pl.ds(pl.multiple_of(h * 128, 128), 128)]
                gr = gt[pl.ds(h, 1), rows]
                gap = jnp.concatenate([gc, gc], axis=1) - gr
                m = (jnp.exp2(jnp.minimum(gap, 0.0)) * cb).astype(BF16)
                ys.append(dot(m, up))
            ybuf[rows, pl.ds(off, 128)] = jnp.where(lane < 64, ys[0], ys[1])
            return 0

        lax.fori_loop(lo, hi, pair, 0)

    local_pairs(0, 0, 12)

    for j in range(8):
        @pl.when(j != g)
        def _(j=j):
            landed(tr.at[j], at_recv.at[j])
            landed(rs.at[j], a_recv.at[j])
    e128 = one_hot((128, wid), 64)

    def table(ref):
        t = jnp.concatenate([ref[j, 0:1, :] for j in range(8)], axis=0)
        return t

    def spread(t):
        p = parts_of(t, 3)
        return dot(p[0], e128) + dot(p[1], e128) + dot(p[2], e128)

    tt = table(tr)
    dec = spread(jnp.exp2(tt))
    run = jnp.zeros((16, wid), F32)
    dr = jnp.ones((1, wid), F32)
    for j in range(8):
        pref[j] = run
        dpre[j:j + 1] = dr
        run = run * dec[j:j + 1] + rs[j].astype(F32)
        dr = dr * dec[j:j + 1]
    rowst[...] = run.astype(BF16)
    rtst[...] = jnp.broadcast_to(jnp.sum(tt, axis=0, keepdims=True), (8, 128))
    for d in range(1, 8):
        @pl.when(row + d < 8)
        def _(d=d):
            rt_copy(d).start()
            r_copy(d).start()

    local_pairs(1, 0, 8)

    for r in range(7):
        @pl.when(r < row)
        def _(r=r):
            landed(rtr.at[r], rt_recv.at[r])
            landed(rr.at[r], r_recv.at[r])
    rmask = lax.broadcasted_iota(jnp.int32, (8, 128), 0) < row
    rdec = spread(jnp.where(rmask, jnp.exp2(table(rtr)), 0.0))
    rc = jnp.zeros((16, wid), F32)
    for r in range(7):
        rc = jnp.where(r < row, rc * rdec[r:r + 1] + rr[r].astype(F32), rc)
    for j in range(8):
        back[j] = (pref[j] + dpre[j:j + 1] * rc).astype(BF16)
    for d in (4, 5, 3, 2, 6, 1, 7):
        c_copy(lax.rem(g + d, 8)).start()
    cin[slice_of(g), :] = back[g]

    local_pairs(1, 8, 12)

    skip = expand(jnp.broadcast_to(skip_ref[...], (8, nh)))[0:1]
    et = jnp.where(lax.broadcasted_iota(jnp.int32, (wid, nh), 0) // 64
                   == lax.broadcasted_iota(jnp.int32, (wid, nh), 1), 1.0, 0.0).astype(BF16)
    for j in range(8):
        @pl.when(j != g)
        def _(j=j):
            landed(cin.at[pl.ds(j * 16, 16)], c_recv.at[j])
    entering = cin[...].astype(F32)
    for c in range(2):
        rows = slice(c * blk, (c + 1) * blk)
        if c == 1:
            entering = eexp[blk - 1:blk] * entering + s0[...]
        y = ybuf[rows] + eexp[rows] * dot(c_ref[rows], entering.astype(BF16))
        y = y + skip * x_ref[rows].astype(F32)
        sq = parts_of(y * y, 2)
        ssum = dot(sq[0], et) + dot(sq[1], et)
        inv = lax.rsqrt(ssum * (1.0 / 64.0) + EPSILON)
        n_ref[rows] = (y * expand(inv) * hg_ref[...].reshape(1, wid)).astype(BF16)

    for d in range(1, 8):
        at_copy(d).wait_send()
        a_copy(d).wait_send()
        c_copy(lax.rem(g + d, 8)).wait_send()

        @pl.when(row + d < 8)
        def _(d=d):
            rt_copy(d).wait_send()
            r_copy(d).wait_send()


def mixer(x, b, c, step, ld, skip, hg):
    V = pltpu.VMEM
    D = pltpu.SemaphoreType.DMA
    wid = 1536
    return pl.pallas_call(
        mixer_kernel,
        name="mixer",
        out_shape=jax.ShapeDtypeStruct((512, wid), BF16),
        in_specs=[pl.BlockSpec(memory_space=V)] * 7,
        out_specs=pl.BlockSpec(memory_space=V),
        scratch_shapes=[
            V((512, wid), BF16), V((512, wid), F32), V((512, wid), F32), V((512, 3072), F32),
            V((24, 512), F32), V((128, wid), F32), V((128, wid), BF16), V((8, 16, wid), BF16),
            V((8, 16, wid), F32), V((8, wid), F32), V((16, wid), BF16), V((8, 16, wid), BF16),
            V((8, 16, wid), BF16), V((128, wid), BF16),
            V((8, 128), F32), V((8, 8, 128), F32), V((8, 128), F32), V((8, 8, 128), F32),
        ] + [D((8,))] * 10,
        compiler_params=pltpu.CompilerParams(
            collective_id=1, has_side_effects=True, vmem_limit_bytes=60 * 2**20),
    )(x, b, c, step.T, ld.T, skip.reshape(1, 24), hg)

def back_kernel(n_ref, res_ref, wo_hbm, wq_hbm, gain_ref, stream_ref, out_ref,
                wo_p, wo_o, wq, base, psend, precv, srecv,
                own, buf, knat, osend, oland, mkeep, lkeep, akeep,
                w_sem, p_send, p_recv, s_send, s_recv,
                send_sem, recv_sem, qsend_sem, qrecv_sem, hsend_sem, hrecv_sem, osend_sem, orecv_sem):
    z = lax.axis_index("seq_0")
    yh = lax.axis_index("seq_1")
    xx = lax.axis_index("seq_2")
    cc = lax.axis_index("seq_3")
    tp = lax.axis_index("tp")
    g = xx * 2 + cc
    row = z * 2 + yh
    nrow = lax.rem(row + 1, 8)
    prow = lax.rem(row + 7, 8)
    hd, tok, ch, nch, half = 96, 512, 128, 4, 1536

    def at_group(j):
        return {"seq_2": j // 2, "seq_3": lax.rem(j, 2)}

    def at_row(r):
        return {"seq_0": r // 2, "seq_1": lax.rem(r, 2)}

    partner = {"tp": 1 - tp}
    own_cols = pl.ds(pl.multiple_of(tp * half, half), half)
    far_cols = pl.ds(pl.multiple_of((1 - tp) * half, half), half)

    def dot(a, b):
        return jnp.dot(a, b, preferred_element_type=F32)

    loads = [
        pltpu.make_async_copy(wo_hbm.at[:, far_cols], wo_p, w_sem.at[0]),
        pltpu.make_async_copy(wo_hbm.at[:, own_cols], wo_o, w_sem.at[1]),
        pltpu.make_async_copy(wq_hbm, wq, w_sem.at[2]),
    ]
    for load in loads:
        load.start()

    barrier = pltpu.get_barrier_semaphore()
    for d in range(1, 8):
        pl.semaphore_signal(barrier, inc=1, device_id=at_group(lax.rem(g + d, 8)), device_id_type=MESH)
    for dev in (at_row(nrow), at_row(prow), partner):
        pl.semaphore_signal(barrier, inc=1, device_id=dev, device_id_type=MESH)
    def rows(c):
        return slice(c * ch, (c + 1) * ch)

    def p_copy(c):
        return pltpu.make_async_remote_copy(
            src_ref=psend.at[c], dst_ref=precv.at[c], send_sem=p_send.at[c],
            recv_sem=p_recv.at[c], device_id=partner, device_id_type=MESH)

    def s_copy(c):
        return pltpu.make_async_remote_copy(
            src_ref=stream_ref.at[pl.ds(c * ch, ch)], dst_ref=srecv.at[c], send_sem=s_send.at[c],
            recv_sem=s_recv.at[c], device_id=partner, device_id_type=MESH)

    def project(c):
        psend[c] = dot(n_ref[rows(c)], wo_p[...]).astype(BF16)

    def add_up(c):
        p_copy(c).wait_recv()
        stream_ref[rows(c)] = (base[rows(c)] + precv[c].astype(F32)).astype(BF16)
        s_copy(c).start()

    loads[0].wait()
    project(0)
    pl.semaphore_wait(barrier, 10)
    p_copy(0).start()
    project(1)
    p_copy(1).start()
    loads[1].wait()
    for c in range(nch):
        base[rows(c)] = res_ref[rows(c)].astype(F32) + dot(n_ref[rows(c)], wo_o[...])
    project(2)
    project(3)
    for c in range(2):
        add_up(c)
        p_copy(c + 2).start()
    loads[2].wait()

    def head(j):
        return pl.ds(pl.multiple_of(j * hd, 32), hd)

    def kv_copy(c, d):
        j = lax.rem(g + d, 8)
        return pltpu.make_async_remote_copy(
            src_ref=own.at[c, pl.ds(1, 2), head(j), :],
            dst_ref=buf.at[4 + g, c, pl.ds(1, 2)],
            send_sem=send_sem.at[c, d],
            recv_sem=recv_sem.at[c, g],
            device_id=at_group(j), device_id_type=MESH)

    def q_copy(c, d):
        j = lax.rem(g + d, 8)
        return pltpu.make_async_remote_copy(
            src_ref=own.at[c, 0, head(j), :],
            dst_ref=buf.at[4 + g, c, 0],
            send_sem=qsend_sem.at[c, d],
            recv_sem=qrecv_sem.at[c, g],
            device_id=at_group(j), device_id_type=MESH)

    def halo_copy(c, i):
        return pltpu.make_async_remote_copy(
            src_ref=buf.at[8 + i, c, pl.ds(1, 2)],
            dst_ref=buf.at[i, c, pl.ds(1, 2)],
            send_sem=hsend_sem.at[c, i],
            recv_sem=hrecv_sem.at[c, i],
            device_id=at_row(nrow), device_id_type=MESH)

    def out_copy(b):
        return pltpu.make_async_remote_copy(
            src_ref=osend.at[b],
            dst_ref=oland.at[g],
            send_sem=osend_sem.at[b],
            recv_sem=orecv_sem.at[g],
            device_id=at_group(b), device_id_type=MESH)

    def landed(ref, sem):
        pltpu.make_async_copy(ref, ref, sem).wait()

    def arrivals(c):
        for b in (4, 5, 6, 7, 0, 1, 2, 3):
            @pl.when(b != g)
            def _(b=b):
                landed(buf.at[4 + b, c, pl.ds(1, 2)], recv_sem.at[c, b])
            if b >= 4:
                @pl.when(row < 7)
                def _(b=b):
                    halo_copy(c, b - 4).start()
        for b in range(8):
            knat[4 + b, c * ch:(c + 1) * ch, :] = buf[4 + b, c, 1].T
        for b in range(8):
            @pl.when(b != g)
            def _(b=b):
                landed(buf.at[4 + b, c, 0], qrecv_sem.at[c, b])

    gain_own = gain_ref[own_cols].reshape(1, half)
    gain_far = gain_ref[far_cols].reshape(1, half)
    for c in range(nch):
        landed(srecv.at[c], s_recv.at[c])
        a = stream_ref[rows(c)].astype(F32)
        f = srecv[c].astype(F32)
        ss = jnp.sum(a * a, axis=1, keepdims=True) + jnp.sum(f * f, axis=1, keepdims=True)
        inv = lax.rsqrt(ss * (1.0 / (2 * half)) + EPSILON)
        na = (a * inv * gain_own).astype(BF16)
        nf = (f * inv * gain_far).astype(BF16)
        for i in (1, 2, 0):
            r = dot(na, wq[i, own_cols, :]) + dot(nf, wq[i, far_cols, :])
            own[c, i] = r.astype(BF16).T
            for d in (4, 5, 3, 2, 6, 1, 7):
                if i == 2:
                    kv_copy(c, d).start()
                if i == 0:
                    q_copy(c, d).start()
        buf[4 + g, c] = own[c, :, head(g), :]
        if c < 2:
            add_up(c + 2)
        if c > 0:
            arrivals(c - 1)
    scale = (hd ** -0.5) * LOG2E
    early = 3 * ch

    def causal(n):
        return (lax.broadcasted_iota(jnp.int32, (n, n), 0)
                <= lax.broadcasted_iota(jnp.int32, (n, n), 1))

    def wide(j, i, lo, hi):
        return jnp.concatenate([buf[j, c, i] for c in range(lo, hi)], axis=1)

    @pl.when(row == 0)
    def _():
        for i in range(4):
            knat[i] = jnp.zeros((tok, hd), BF16)
            for c in range(nch):
                buf[i, c, 2] = jnp.zeros((hd, ch), BF16)

    def order(step):
        return jnp.where(step < 4, 4 + step, 7 - step)

    def halo_in(step, b, lo, hi):
        @pl.when(jnp.logical_and(step >= 4, row > 0))
        def _():
            for c in range(lo, hi):
                halo_copy(c, b).wait_recv()
                knat[b, c * ch:(c + 1) * ch, :] = buf[b, c, 1].T

    low = causal(early)

    def first_round(step, _):
        b = order(step)
        halo_in(step, b, 0, 3)
        qt = wide(4 + b, 0, 0, 3)
        has_far = jnp.logical_or(step < 4, row > 0)
        s_diag = dot(knat[4 + b, 0:early], qt)
        s_far = dot(knat[b, 0:early], qt)
        s = jnp.where(low, s_diag, jnp.where(has_far, s_far, NEG))
        m = jnp.max(s, axis=0, keepdims=True)
        p = jnp.exp2((s - m) * scale)
        l = jnp.sum(p, axis=0, keepdims=True)
        acc = dot(wide(4 + b, 2, 0, 3), jnp.where(low, p, 0.0).astype(BF16))
        acc = acc + dot(wide(b, 2, 0, 3), jnp.where(low, 0.0, p).astype(BF16))

        def mid(j, carry):
            m, l, acc = carry
            s = dot(knat[j, 0:early], qt)
            m_new = jnp.maximum(m, jnp.max(s, axis=0, keepdims=True))
            alpha = jnp.exp2((m - m_new) * scale)
            p = jnp.exp2((s - m_new) * scale)
            l = alpha * l + jnp.sum(p, axis=0, keepdims=True)
            acc = alpha * acc + dot(wide(j, 2, 0, 3), p.astype(BF16))
            return m_new, l, acc

        first = jnp.where(row > 0, b + 1, jnp.maximum(b + 1, 4))
        m, l, acc = lax.fori_loop(first, b + 4, mid, (m, l, acc))
        mkeep[b] = m
        lkeep[b] = l
        akeep[b] = acc
        return 0

    lax.fori_loop(0, 8, first_round, 0)
    arrivals(nch - 1)
    low1 = causal(ch)

    def second_round(step, _):
        b = order(step)
        halo_in(step, b, 3, 4)

        def there(i):
            return jnp.logical_or(b + i >= 4, row > 0)

        qt = wide(4 + b, 0, 0, 3)
        ss = [jnp.where(there(i), dot(knat[b + i, early:tok], qt), NEG) for i in range(4)]
        m = mkeep[b]
        m_new = m
        for t in ss:
            m_new = jnp.maximum(m_new, jnp.max(t, axis=0, keepdims=True))
        alpha = jnp.exp2((m - m_new) * scale)
        ps = [jnp.exp2((t - m_new) * scale) for t in ss]
        l = alpha * lkeep[b]
        for t in ps:
            l = l + jnp.sum(t, axis=0, keepdims=True)
        pt = jnp.concatenate([t.astype(BF16) for t in ps], axis=0)
        vt = jnp.concatenate([buf[b + i, 3, 2] for i in range(4)], axis=1)
        acc = alpha * akeep[b] + dot(vt, pt)
        osend[b, :, 0:early] = (acc / l).astype(BF16)

        qt = buf[4 + b, 3, 0]
        s_diag = dot(knat[4 + b, early:tok], qt)
        s_far = dot(knat[b, early:tok], qt)
        ss = [jnp.where(low1, s_diag, jnp.where(there(0), s_far, NEG)), dot(knat[4 + b, 0:early], qt)]
        ss += [jnp.where(there(i), dot(knat[b + i], qt), NEG) for i in range(1, 4)]
        m = jnp.max(ss[0], axis=0, keepdims=True)
        for t in ss[1:]:
            m = jnp.maximum(m, jnp.max(t, axis=0, keepdims=True))
        ps = [jnp.exp2((t - m) * scale) for t in ss]
        l = jnp.sum(ps[0], axis=0, keepdims=True)
        for t in ps[1:]:
            l = l + jnp.sum(t, axis=0, keepdims=True)
        pt = jnp.concatenate(
            [jnp.where(low1, ps[0], 0.0).astype(BF16), jnp.where(low1, 0.0, ps[0]).astype(BF16)]
            + [t.astype(BF16) for t in ps[1:]], axis=0)
        vt = jnp.concatenate(
            [buf[4 + b, 3, 2], buf[b, 3, 2], wide(4 + b, 2, 0, 3)]
            + [wide(b + i, 2, 0, 4) for i in range(1, 4)], axis=1)
        osend[b, :, early:tok] = (dot(vt, pt) / l).astype(BF16)

        @pl.when(b != g)
        def _():
            out_copy(b).start()
        return 0

    lax.fori_loop(0, 8, second_round, 0)
    oland[g] = osend[g]
    for b in range(8):
        @pl.when(b != g)
        def _(b=b):
            landed(oland.at[b], orecv_sem.at[b])
    out_ref[...] = oland[...].reshape(8 * hd, tok).T
    for c in range(nch):
        p_copy(c).wait_send()
        s_copy(c).wait_send()
        for d in range(1, 8):
            kv_copy(c, d).wait_send()
            q_copy(c, d).wait_send()
    for b in range(8):
        @pl.when(b != g)
        def _(b=b):
            out_copy(b).wait_send()

    @pl.when(row < 7)
    def _():
        for c in range(nch):
            for i in range(4):
                halo_copy(c, i).wait_send()


def back(normed, residual, mixer_out, weight, gain):
    V = pltpu.VMEM
    D = pltpu.SemaphoreType.DMA
    vm = pl.BlockSpec(memory_space=V)
    hbm = pl.BlockSpec(memory_space=pl.ANY)
    return pl.pallas_call(
        back_kernel,
        name="back",
        out_shape=(jax.ShapeDtypeStruct((512, 1536), BF16), jax.ShapeDtypeStruct((512, 768), BF16)),
        in_specs=[vm, vm, hbm, hbm, vm],
        out_specs=(vm, vm),
        scratch_shapes=[
            V((1536, 1536), BF16), V((1536, 1536), BF16), V((3, 3072, 768), BF16),
            V((512, 1536), F32), V((4, 128, 1536), BF16), V((4, 128, 1536), BF16), V((4, 128, 1536), BF16),
            V((4, 3, 768, 128), BF16), V((12, 4, 3, 96, 128), BF16), V((12, 512, 96), BF16),
            V((8, 96, 512), BF16), V((8, 96, 512), BF16),
            V((8, 1, 384), F32), V((8, 1, 384), F32), V((8, 96, 384), F32),
            D((3,)), D((4,)), D((4,)), D((4,)), D((4,)),
            D((4, 8)), D((4, 8)), D((4, 8)), D((4, 8)), D((4, 4)), D((4, 4)), D((8,)), D((8,)),
        ],
        compiler_params=pltpu.CompilerParams(
            collective_id=2, has_side_effects=True, vmem_limit_bytes=54 * 2**20),
    )(normed, residual, mixer_out, weight, gain)


def on_device(
    mixer_input,
    state_write,
    state_read,
    step_size,
    log_decay,
    skip_gain,
    head_gain,
    mixer_out,
    residual,
    attn_gain,
    qkv_weight,
):
    normed = mixer(mixer_input, state_write, state_read, step_size, log_decay, skip_gain, head_gain)
    weight = jnp.transpose(qkv_weight, (1, 0, 2))
    stream, pieces = back(normed, residual, mixer_out, weight, attn_gain)
    return (stream, pieces)


def solution(mesh):
    torus = Mesh(
        mesh.devices.reshape(4, 2, 4, 2, mesh.shape["tp"]),
        ("seq_0", "seq_1", "seq_2", "seq_3", "tp"),
    )
    in_specs = (
        P(SEQ, "tp"),
        P(SEQ, None),
        P(SEQ, None),
        P(SEQ, "tp"),
        P(SEQ, "tp"),
        P("tp"),
        P("tp"),
        P("tp", None),
        P(SEQ, "tp"),
        P(),
        P(None, None, "tp"),
    )
    out_specs = (P(SEQ, "tp"), P(SEQ, "tp"))
    return jax.shard_map(
        on_device, mesh=torus, in_specs=in_specs, out_specs=out_specs, check_vma=False
    )
```

```python
import jax
import jax.numpy as jnp
from jax import lax
from jax.sharding import Mesh
from jax.experimental import pallas as pl
from jax.experimental.pallas import tpu as pltpu
from jax.sharding import PartitionSpec as P

SEQ = ("seq_0", "seq_1", "seq_2", "seq_3")


EPSILON = 1e-05


MESH = pl.DeviceIdType.MESH
F32 = jnp.float32
BF16 = jnp.bfloat16
NEG = -1e30
LOG2E = 1.4426950408889634


def parts_of(v, count):
    out = []
    for _ in range(count):
        piece = v.astype(BF16)
        out.append(piece)
        v = v - piece.astype(F32)
    return out


def one_hot(shape, per_lane, period=None):
    r = lax.broadcasted_iota(jnp.int32, shape, 0)
    c = lax.broadcasted_iota(jnp.int32, shape, 1)
    if period is not None:
        r = lax.rem(r, period)
    return jnp.where(r == c // per_lane, 1.0, 0.0).astype(BF16)


def mixer_kernel(x_ref, b_ref, c_ref, step_ref, ld_ref, skip_ref, hg_ref, n_ref,
                 u, ybuf, eexp, gexp, gt, s0, stage, rs, pref, dpre, rowst, rr, back, cin,
                 tst, tr, rtst, rtr,
                 a_send, a_recv, at_send, at_recv, r_send, r_recv, rt_send, rt_recv,
                 c_send, c_recv):
    z = lax.axis_index("seq_0")
    yh = lax.axis_index("seq_1")
    xx = lax.axis_index("seq_2")
    cc = lax.axis_index("seq_3")
    g = xx * 2 + cc
    row = z * 2 + yh
    nh, blk, wid = 24, 256, 1536

    def at_group(j):
        return {"seq_2": j // 2, "seq_3": lax.rem(j, 2)}

    def at_row(r):
        return {"seq_0": r // 2, "seq_1": lax.rem(r, 2)}

    barrier = pltpu.get_barrier_semaphore()
    for d in range(1, 8):
        pl.semaphore_signal(barrier, inc=1, device_id=at_group(lax.rem(g + d, 8)), device_id_type=MESH)
        pl.semaphore_signal(barrier, inc=1, device_id=at_row(lax.rem(row + d, 8)), device_id_type=MESH)

    def dot(a, b):
        return jnp.dot(a, b, preferred_element_type=F32)

    si = lax.broadcasted_iota(jnp.int32, (blk, blk), 0)
    ti = lax.broadcasted_iota(jnp.int32, (blk, blk), 1)
    upto = jnp.where(si <= ti, 1.0, 0.0).astype(BF16)
    wt = []
    for c in range(2):
        ld = ld_ref[:, c * blk:(c + 1) * blk]
        cat = jnp.concatenate(parts_of(ld, 3), axis=0)
        r = dot(cat, upto)
        gtc = (r[0:nh] + r[nh:2 * nh] + r[2 * nh:3 * nh]) * LOG2E
        gt[:, c * blk:(c + 1) * blk] = gtc
        wt.append(jnp.exp2(gtc[:, blk - 1:blk] - gtc))
    gtv = gt[...]
    g_col = gtv.T
    total = g_col[blk - 1:blk] + g_col[2 * blk - 1:2 * blk]
    tst[...] = jnp.zeros((8, 128), F32)
    tst[0:1, 0:nh] = total

    e3 = one_hot((3 * nh, wid), 64, nh)

    def expand(v, count=3):
        k = count * nh
        return dot(jnp.concatenate(parts_of(v, count), axis=1), e3[0:k] if count < 3 else e3)

    step_col = step_ref[...].T
    w_col = jnp.concatenate(wt, axis=1).T
    e_col = jnp.exp2(g_col)
    state = None
    for c in range(2):
        rows = slice(c * blk, (c + 1) * blk)
        uc = (expand(step_col[rows]) * x_ref[rows].astype(F32)).astype(BF16)
        u[rows] = uc
        wu = (expand(w_col[rows]) * uc.astype(F32)).astype(BF16)
        term = dot(b_ref[rows].T, wu)
        if c == 0:
            s0[...] = term
        else:
            state = expand(e_col[2 * blk - 8:2 * blk])[7:8] * s0[...] + term
    stage[...] = state.astype(BF16)
    pl.semaphore_wait(barrier, 14)

    def slice_of(j):
        return pl.ds(pl.multiple_of(j * 16, 16), 16)

    def a_copy(d):
        j = lax.rem(g + d, 8)
        return pltpu.make_async_remote_copy(
            src_ref=stage.at[slice_of(j)], dst_ref=rs.at[g],
            send_sem=a_send.at[d], recv_sem=a_recv.at[g],
            device_id=at_group(j), device_id_type=MESH)

    def at_copy(d):
        j = lax.rem(g + d, 8)
        return pltpu.make_async_remote_copy(
            src_ref=tst, dst_ref=tr.at[g],
            send_sem=at_send.at[d], recv_sem=at_recv.at[g],
            device_id=at_group(j), device_id_type=MESH)

    def r_copy(d):
        return pltpu.make_async_remote_copy(
            src_ref=rowst, dst_ref=rr.at[row],
            send_sem=r_send.at[d], recv_sem=r_recv.at[row],
            device_id=at_row(lax.rem(row + d, 8)), device_id_type=MESH)

    def rt_copy(d):
        return pltpu.make_async_remote_copy(
            src_ref=rtst, dst_ref=rtr.at[row],
            send_sem=rt_send.at[d], recv_sem=rt_recv.at[row],
            device_id=at_row(lax.rem(row + d, 8)), device_id_type=MESH)

    def c_copy(j):
        return pltpu.make_async_remote_copy(
            src_ref=back.at[j], dst_ref=cin.at[slice_of(g)],
            send_sem=c_send.at[j], recv_sem=c_recv.at[g],
            device_id=at_group(j), device_id_type=MESH)

    def landed(ref, sem):
        pltpu.make_async_copy(ref, ref, sem).wait()

    for d in range(1, 8):
        at_copy(d).start()
    for d in (4, 5, 3, 2, 6, 1, 7):
        a_copy(d).start()
    rs[g] = stage[slice_of(g), :]
    tr[g] = tst[...]
    one3 = one_hot((3 * nh, nh * 128), 128, nh)
    gexp[...] = dot(jnp.concatenate(parts_of(g_col, 3), axis=1), one3)
    eexp[...] = expand(e_col)

    causal = si >= ti

    def local_pairs(c, lo, hi):
        rows = slice(c * blk, (c + 1) * blk)
        cb = lax.dot_general(c_ref[rows], b_ref[rows], (((1,), (1,)), ((), ())),
                             preferred_element_type=F32)
        cb = jnp.where(causal, cb, 0.0)
        lane = lax.broadcasted_iota(jnp.int32, (blk, 128), 1)

        def pair(p, _):
            off = pl.multiple_of(p * 128, 128)
            up = u[rows, pl.ds(off, 128)]
            ys = []
            for k in range(2):
                h = p * 2 + k
                gc = gexp[rows, pl.ds(pl.multiple_of(h * 128, 128), 128)]
                gr = gt[pl.ds(h, 1), rows]
                gap = jnp.concatenate([gc, gc], axis=1) - gr
                m = (jnp.exp2(jnp.minimum(gap, 0.0)) * cb).astype(BF16)
                ys.append(dot(m, up))
            ybuf[rows, pl.ds(off, 128)] = jnp.where(lane < 64, ys[0], ys[1])
            return 0

        lax.fori_loop(lo, hi, pair, 0)

    local_pairs(0, 0, 12)

    for j in range(8):
        @pl.when(j != g)
        def _(j=j):
            landed(tr.at[j], at_recv.at[j])
            landed(rs.at[j], a_recv.at[j])
    e128 = one_hot((128, wid), 64)

    def table(ref):
        t = jnp.concatenate([ref[j, 0:1, :] for j in range(8)], axis=0)
        return t

    def spread(t):
        p = parts_of(t, 3)
        return dot(p[0], e128) + dot(p[1], e128) + dot(p[2], e128)

    tt = table(tr)
    dec = spread(jnp.exp2(tt))
    run = jnp.zeros((16, wid), F32)
    dr = jnp.ones((1, wid), F32)
    for j in range(8):
        pref[j] = run
        dpre[j:j + 1] = dr
        run = run * dec[j:j + 1] + rs[j].astype(F32)
        dr = dr * dec[j:j + 1]
    rowst[...] = run.astype(BF16)
    rtst[...] = jnp.broadcast_to(jnp.sum(tt, axis=0, keepdims=True), (8, 128))
    for d in range(1, 8):
        @pl.when(row + d < 8)
        def _(d=d):
            rt_copy(d).start()
            r_copy(d).start()

    local_pairs(1, 0, 8)

    for r in range(7):
        @pl.when(r < row)
        def _(r=r):
            landed(rtr.at[r], rt_recv.at[r])
            landed(rr.at[r], r_recv.at[r])
    rmask = lax.broadcasted_iota(jnp.int32, (8, 128), 0) < row
    rdec = spread(jnp.where(rmask, jnp.exp2(table(rtr)), 0.0))
    rc = jnp.zeros((16, wid), F32)
    for r in range(7):
        rc = jnp.where(r < row, rc * rdec[r:r + 1] + rr[r].astype(F32), rc)
    for j in range(8):
        back[j] = (pref[j] + dpre[j:j + 1] * rc).astype(BF16)
    for d in (4, 5, 3, 2, 6, 1, 7):
        c_copy(lax.rem(g + d, 8)).start()
    cin[slice_of(g), :] = back[g]

    local_pairs(1, 8, 12)

    skip = expand(jnp.broadcast_to(skip_ref[...], (8, nh)))[0:1]
    et = jnp.where(lax.broadcasted_iota(jnp.int32, (wid, nh), 0) // 64
                   == lax.broadcasted_iota(jnp.int32, (wid, nh), 1), 1.0, 0.0).astype(BF16)
    for j in range(8):
        @pl.when(j != g)
        def _(j=j):
            landed(cin.at[pl.ds(j * 16, 16)], c_recv.at[j])
    entering = cin[...].astype(F32)
    for c in range(2):
        rows = slice(c * blk, (c + 1) * blk)
        if c == 1:
            entering = eexp[blk - 1:blk] * entering + s0[...]
        y = ybuf[rows] + eexp[rows] * dot(c_ref[rows], entering.astype(BF16))
        y = y + skip * x_ref[rows].astype(F32)
        sq = parts_of(y * y, 2)
        ssum = dot(sq[0], et) + dot(sq[1], et)
        inv = lax.rsqrt(ssum * (1.0 / 64.0) + EPSILON)
        n_ref[rows] = (y * expand(inv) * hg_ref[...].reshape(1, wid)).astype(BF16)

    for d in range(1, 8):
        at_copy(d).wait_send()
        a_copy(d).wait_send()
        c_copy(lax.rem(g + d, 8)).wait_send()

        @pl.when(row + d < 8)
        def _(d=d):
            rt_copy(d).wait_send()
            r_copy(d).wait_send()


def mixer(x, b, c, step, ld, skip, hg):
    V = pltpu.VMEM
    D = pltpu.SemaphoreType.DMA
    wid = 1536
    return pl.pallas_call(
        mixer_kernel,
        name="mixer",
        out_shape=jax.ShapeDtypeStruct((512, wid), BF16),
        in_specs=[pl.BlockSpec(memory_space=V)] * 7,
        out_specs=pl.BlockSpec(memory_space=V),
        scratch_shapes=[
            V((512, wid), BF16), V((512, wid), F32), V((512, wid), F32), V((512, 3072), F32),
            V((24, 512), F32), V((128, wid), F32), V((128, wid), BF16), V((8, 16, wid), BF16),
            V((8, 16, wid), F32), V((8, wid), F32), V((16, wid), BF16), V((8, 16, wid), BF16),
            V((8, 16, wid), BF16), V((128, wid), BF16),
            V((8, 128), F32), V((8, 8, 128), F32), V((8, 128), F32), V((8, 8, 128), F32),
        ] + [D((8,))] * 10,
        compiler_params=pltpu.CompilerParams(
            collective_id=1, has_side_effects=True, vmem_limit_bytes=60 * 2**20),
    )(x, b, c, step.T, ld.T, skip.reshape(1, 24), hg)

def back_kernel(n_ref, res_ref, wo_hbm, wq_hbm, gain_ref, stream_ref, out_ref,
                wo_p, wo_o, wq, base, psend, precv, srecv,
                own, buf, knat, osend, oland, mkeep, lkeep, akeep,
                w_sem, p_send, p_recv, s_send, s_recv,
                send_sem, recv_sem, qsend_sem, qrecv_sem, hsend_sem, hrecv_sem, osend_sem, orecv_sem):
    z = lax.axis_index("seq_0")
    yh = lax.axis_index("seq_1")
    xx = lax.axis_index("seq_2")
    cc = lax.axis_index("seq_3")
    tp = lax.axis_index("tp")
    g = xx * 2 + cc
    row = z * 2 + yh
    nrow = lax.rem(row + 1, 8)
    prow = lax.rem(row + 7, 8)
    hd, tok, ch, nch, half = 96, 512, 128, 4, 1536

    def at_group(j):
        return {"seq_2": j // 2, "seq_3": lax.rem(j, 2)}

    def at_row(r):
        return {"seq_0": r // 2, "seq_1": lax.rem(r, 2)}

    partner = {"tp": 1 - tp}
    own_cols = pl.ds(pl.multiple_of(tp * half, half), half)
    far_cols = pl.ds(pl.multiple_of((1 - tp) * half, half), half)

    def dot(a, b):
        return jnp.dot(a, b, preferred_element_type=F32)

    loads = [
        pltpu.make_async_copy(wo_hbm.at[:, far_cols], wo_p, w_sem.at[0]),
        pltpu.make_async_copy(wo_hbm.at[:, own_cols], wo_o, w_sem.at[1]),
        pltpu.make_async_copy(wq_hbm, wq, w_sem.at[2]),
    ]
    for load in loads:
        load.start()

    barrier = pltpu.get_barrier_semaphore()
    for d in range(1, 8):
        pl.semaphore_signal(barrier, inc=1, device_id=at_group(lax.rem(g + d, 8)), device_id_type=MESH)
    for dev in (at_row(nrow), at_row(prow), partner):
        pl.semaphore_signal(barrier, inc=1, device_id=dev, device_id_type=MESH)
    def rows(c):
        return slice(c * ch, (c + 1) * ch)

    def p_copy(c):
        return pltpu.make_async_remote_copy(
            src_ref=psend.at[c], dst_ref=precv.at[c], send_sem=p_send.at[c],
            recv_sem=p_recv.at[c], device_id=partner, device_id_type=MESH)

    def s_copy(c):
        return pltpu.make_async_remote_copy(
            src_ref=stream_ref.at[pl.ds(c * ch, ch)], dst_ref=srecv.at[c], send_sem=s_send.at[c],
            recv_sem=s_recv.at[c], device_id=partner, device_id_type=MESH)

    def project(c):
        psend[c] = dot(n_ref[rows(c)], wo_p[...]).astype(BF16)

    def add_up(c):
        p_copy(c).wait_recv()
        stream_ref[rows(c)] = (base[rows(c)] + precv[c].astype(F32)).astype(BF16)
        s_copy(c).start()

    loads[0].wait()
    project(0)
    pl.semaphore_wait(barrier, 10)
    p_copy(0).start()
    project(1)
    p_copy(1).start()
    loads[1].wait()
    for c in range(nch):
        base[rows(c)] = res_ref[rows(c)].astype(F32) + dot(n_ref[rows(c)], wo_o[...])
    project(2)
    project(3)
    for c in range(2):
        add_up(c)
        p_copy(c + 2).start()
    loads[2].wait()

    def head(j):
        return pl.ds(pl.multiple_of(j * hd, 32), hd)

    def kv_copy(c, d):
        j = lax.rem(g + d, 8)
        return pltpu.make_async_remote_copy(
            src_ref=own.at[c, pl.ds(1, 2), head(j), :],
            dst_ref=buf.at[4 + g, c, pl.ds(1, 2)],
            send_sem=send_sem.at[c, d],
            recv_sem=recv_sem.at[c, g],
            device_id=at_group(j), device_id_type=MESH)

    def q_copy(c, d):
        j = lax.rem(g + d, 8)
        return pltpu.make_async_remote_copy(
            src_ref=own.at[c, 0, head(j), :],
            dst_ref=buf.at[4 + g, c, 0],
            send_sem=qsend_sem.at[c, d],
            recv_sem=qrecv_sem.at[c, g],
            device_id=at_group(j), device_id_type=MESH)

    def halo_copy(c, i):
        return pltpu.make_async_remote_copy(
            src_ref=buf.at[8 + i, c, pl.ds(1, 2)],
            dst_ref=buf.at[i, c, pl.ds(1, 2)],
            send_sem=hsend_sem.at[c, i],
            recv_sem=hrecv_sem.at[c, i],
            device_id=at_row(nrow), device_id_type=MESH)

    def out_copy(b):
        return pltpu.make_async_remote_copy(
            src_ref=osend.at[b],
            dst_ref=oland.at[g],
            send_sem=osend_sem.at[b],
            recv_sem=orecv_sem.at[g],
            device_id=at_group(b), device_id_type=MESH)

    def landed(ref, sem):
        pltpu.make_async_copy(ref, ref, sem).wait()

    def arrivals(c):
        for b in (4, 5, 6, 7, 0, 1, 2, 3):
            @pl.when(b != g)
            def _(b=b):
                landed(buf.at[4 + b, c, pl.ds(1, 2)], recv_sem.at[c, b])
            if b >= 4:
                @pl.when(row < 7)
                def _(b=b):
                    halo_copy(c, b - 4).start()
        for b in range(8):
            knat[4 + b, c * ch:(c + 1) * ch, :] = buf[4 + b, c, 1].T
        for b in range(8):
            @pl.when(b != g)
            def _(b=b):
                landed(buf.at[4 + b, c, 0], qrecv_sem.at[c, b])

    scale = (hd ** -0.5) * LOG2E
    early = 2 * ch
    low = (lax.broadcasted_iota(jnp.int32, (early, early), 0)
           <= lax.broadcasted_iota(jnp.int32, (early, early), 1))

    def wide(j, i, lo, hi):
        return jnp.concatenate([buf[j, c, i] for c in range(lo, hi)], axis=1)

    @pl.when(row == 0)
    def _():
        for i in range(4):
            knat[i] = jnp.zeros((tok, hd), BF16)
            for c in range(nch):
                buf[i, c, 2] = jnp.zeros((hd, ch), BF16)

    def order(step):
        return jnp.where(step < 4, 4 + step, 7 - step)

    def halo_in(step, b, lo, hi):
        @pl.when(jnp.logical_and(step >= 4, row > 0))
        def _():
            for c in range(lo, hi):
                halo_copy(c, b).wait_recv()
                knat[b, c * ch:(c + 1) * ch, :] = buf[b, c, 1].T

    def top(tiles):
        m = None
        for t, ok in tiles:
            r = jnp.max(t, axis=0, keepdims=True)
            if ok is not None:
                r = jnp.where(ok, r, NEG)
            m = r if m is None else jnp.maximum(m, r)
        return m

    def powers(tiles, m):
        ps = [jnp.exp2(t - (m if ok is None else jnp.where(ok, m, -NEG))) for t, ok in tiles]
        l = jnp.sum(ps[0], axis=0, keepdims=True)
        for t in ps[1:]:
            l = l + jnp.sum(t, axis=0, keepdims=True)
        return ps, l

    def square(b, lo, hi, qt, far):
        s_diag = dot(knat[4 + b, lo:hi], qt)
        s_far = dot(knat[b, lo:hi], qt)
        return jnp.where(low, s_diag, jnp.where(far, s_far, NEG))

    def halves(p):
        return [jnp.where(low, p, 0.0).astype(BF16), jnp.where(low, 0.0, p).astype(BF16)]

    def there(b, i):
        return jnp.logical_or(b + i >= 4, row > 0)

    def first_round(step, _):
        b = order(step)
        halo_in(step, b, 0, 2)
        qt = wide(4 + b, 0, 0, 2)
        tiles = [(square(b, 0, early, qt, there(b, 0)), None)]
        tiles += [(dot(knat[b + i, 0:early], qt), there(b, i)) for i in range(1, 4)]
        m = top(tiles)
        ps, l = powers(tiles, m)
        pt = jnp.concatenate(halves(ps[0]) + [t.astype(BF16) for t in ps[1:]], axis=0)
        vt = jnp.concatenate([wide(j, 2, 0, 2) for j in (4 + b, b, b + 1, b + 2, b + 3)], axis=1)
        mkeep[b] = m
        lkeep[b] = l
        akeep[b] = dot(vt, pt)
        return 0

    def second_round(step, _):
        b = order(step)
        halo_in(step, b, 2, 4)

        qt = wide(4 + b, 0, 0, 2)
        tiles = [(dot(knat[b + i, early:tok], qt), there(b, i)) for i in range(4)]
        m = mkeep[b]
        m_new = jnp.maximum(m, top(tiles))
        alpha = jnp.exp2(m - m_new)
        ps, l = powers(tiles, m_new)
        l = alpha * lkeep[b] + l
        pt = jnp.concatenate([t.astype(BF16) for t in ps], axis=0)
        vt = jnp.concatenate([wide(b + i, 2, 2, 4) for i in range(4)], axis=1)
        osend[b, :, 0:early] = ((alpha * akeep[b] + dot(vt, pt)) / l).astype(BF16)

        qt = wide(4 + b, 0, 2, 4)
        tiles = [(square(b, early, tok, qt, there(b, 0)), None), (dot(knat[4 + b, 0:early], qt), None)]
        tiles += [(dot(knat[b + i], qt), there(b, i)) for i in range(1, 4)]
        ps, l = powers(tiles, top(tiles))
        pt = jnp.concatenate(halves(ps[0]) + [t.astype(BF16) for t in ps[1:]], axis=0)
        vt = jnp.concatenate(
            [wide(4 + b, 2, 2, 4), wide(b, 2, 2, 4), wide(4 + b, 2, 0, 2)]
            + [wide(b + i, 2, 0, 4) for i in range(1, 4)], axis=1)
        osend[b, :, early:tok] = (dot(vt, pt) / l).astype(BF16)

        @pl.when(b != g)
        def _():
            out_copy(b).start()
        return 0

    gain_own = gain_ref[own_cols].reshape(1, half)
    gain_far = gain_ref[far_cols].reshape(1, half)
    for c in range(nch):
        landed(srecv.at[c], s_recv.at[c])
        a = stream_ref[rows(c)].astype(F32)
        f = srecv[c].astype(F32)
        ss = jnp.sum(a * a, axis=1, keepdims=True) + jnp.sum(f * f, axis=1, keepdims=True)
        inv = lax.rsqrt(ss * (1.0 / (2 * half)) + EPSILON)
        na = (a * inv * gain_own).astype(BF16)
        nf = (f * inv * gain_far).astype(BF16)
        for i in (1, 2, 0):
            r = dot(na, wq[i, own_cols, :]) + dot(nf, wq[i, far_cols, :])
            if i == 0:
                r = r * scale
            own[c, i] = r.astype(BF16).T
            for d in (4, 5, 3, 2, 6, 1, 7):
                if i == 2:
                    kv_copy(c, d).start()
                if i == 0:
                    q_copy(c, d).start()
        buf[4 + g, c] = own[c, :, head(g), :]
        if c < 2:
            add_up(c + 2)
        if c > 0:
            arrivals(c - 1)
        if c == 2:
            lax.fori_loop(0, 8, first_round, 0)
    arrivals(nch - 1)
    lax.fori_loop(0, 8, second_round, 0)
    oland[g] = osend[g]
    for b in range(8):
        @pl.when(b != g)
        def _(b=b):
            landed(oland.at[b], orecv_sem.at[b])
    out_ref[...] = oland[...].reshape(8 * hd, tok).T
    for c in range(nch):
        p_copy(c).wait_send()
        s_copy(c).wait_send()
        for d in range(1, 8):
            kv_copy(c, d).wait_send()
            q_copy(c, d).wait_send()
    for b in range(8):
        @pl.when(b != g)
        def _(b=b):
            out_copy(b).wait_send()

    @pl.when(row < 7)
    def _():
        for c in range(nch):
            for i in range(4):
                halo_copy(c, i).wait_send()


def back(normed, residual, mixer_out, weight, gain):
    V = pltpu.VMEM
    D = pltpu.SemaphoreType.DMA
    vm = pl.BlockSpec(memory_space=V)
    hbm = pl.BlockSpec(memory_space=pl.ANY)
    return pl.pallas_call(
        back_kernel,
        name="back",
        out_shape=(jax.ShapeDtypeStruct((512, 1536), BF16), jax.ShapeDtypeStruct((512, 768), BF16)),
        in_specs=[vm, vm, hbm, hbm, vm],
        out_specs=(vm, vm),
        scratch_shapes=[
            V((1536, 1536), BF16), V((1536, 1536), BF16), V((3, 3072, 768), BF16),
            V((512, 1536), F32), V((4, 128, 1536), BF16), V((4, 128, 1536), BF16), V((4, 128, 1536), BF16),
            V((4, 3, 768, 128), BF16), V((12, 4, 3, 96, 128), BF16), V((12, 512, 96), BF16),
            V((8, 96, 512), BF16), V((8, 96, 512), BF16),
            V((8, 1, 256), F32), V((8, 1, 256), F32), V((8, 96, 256), F32),
            D((3,)), D((4,)), D((4,)), D((4,)), D((4,)),
            D((4, 8)), D((4, 8)), D((4, 8)), D((4, 8)), D((4, 4)), D((4, 4)), D((8,)), D((8,)),
        ],
        compiler_params=pltpu.CompilerParams(
            collective_id=2, has_side_effects=True, vmem_limit_bytes=54 * 2**20),
    )(normed, residual, mixer_out, weight, gain)


def on_device(
    mixer_input,
    state_write,
    state_read,
    step_size,
    log_decay,
    skip_gain,
    head_gain,
    mixer_out,
    residual,
    attn_gain,
    qkv_weight,
):
    normed = mixer(mixer_input, state_write, state_read, step_size, log_decay, skip_gain, head_gain)
    weight = jnp.transpose(qkv_weight, (1, 0, 2))
    stream, pieces = back(normed, residual, mixer_out, weight, attn_gain)
    return (stream, pieces)


def solution(mesh):
    torus = Mesh(
        mesh.devices.reshape(4, 2, 4, 2, mesh.shape["tp"]),
        ("seq_0", "seq_1", "seq_2", "seq_3", "tp"),
    )
    in_specs = (
        P(SEQ, "tp"),
        P(SEQ, None),
        P(SEQ, None),
        P(SEQ, "tp"),
        P(SEQ, "tp"),
        P("tp"),
        P("tp"),
        P("tp", None),
        P(SEQ, "tp"),
        P(),
        P(None, None, "tp"),
    )
    out_specs = (P(SEQ, "tp"), P(SEQ, "tp"))
    return jax.shard_map(
        on_device, mesh=torus, in_specs=in_specs, out_specs=out_specs, check_vma=False
    )
```

```python
import jax
import jax.numpy as jnp
from jax import lax
from jax.sharding import Mesh
from jax.experimental import pallas as pl
from jax.experimental.pallas import tpu as pltpu
from jax.sharding import PartitionSpec as P

SEQ = ("seq_0", "seq_1", "seq_2", "seq_3")


EPSILON = 1e-05


MESH = pl.DeviceIdType.MESH
F32 = jnp.float32
BF16 = jnp.bfloat16
NEG = -1e30
LOG2E = 1.4426950408889634


def parts_of(v, count):
    out = []
    for _ in range(count):
        piece = v.astype(BF16)
        out.append(piece)
        v = v - piece.astype(F32)
    return out


def one_hot(shape, per_lane, period=None):
    r = lax.broadcasted_iota(jnp.int32, shape, 0)
    c = lax.broadcasted_iota(jnp.int32, shape, 1)
    if period is not None:
        r = lax.rem(r, period)
    return jnp.where(r == c // per_lane, 1.0, 0.0).astype(BF16)


def mixer_kernel(x_ref, b_ref, c_ref, step_ref, ld_ref, skip_ref, hg_ref, n_ref,
                 u, ybuf, eexp, gexp, gt, s0, stage, rs, pref, dpre, rowst, rr, back, cin,
                 tst, tr, rtst, rtr,
                 a_send, a_recv, at_send, at_recv, r_send, r_recv, rt_send, rt_recv,
                 c_send, c_recv):
    z = lax.axis_index("seq_0")
    yh = lax.axis_index("seq_1")
    xx = lax.axis_index("seq_2")
    cc = lax.axis_index("seq_3")
    g = xx * 2 + cc
    row = z * 2 + yh
    nh, blk, wid = 24, 256, 1536

    def at_group(j):
        return {"seq_2": j // 2, "seq_3": lax.rem(j, 2)}

    def at_row(r):
        return {"seq_0": r // 2, "seq_1": lax.rem(r, 2)}

    barrier = pltpu.get_barrier_semaphore()
    for d in range(1, 8):
        pl.semaphore_signal(barrier, inc=1, device_id=at_group(lax.rem(g + d, 8)), device_id_type=MESH)
        pl.semaphore_signal(barrier, inc=1, device_id=at_row(lax.rem(row + d, 8)), device_id_type=MESH)

    def dot(a, b):
        return jnp.dot(a, b, preferred_element_type=F32)

    si = lax.broadcasted_iota(jnp.int32, (blk, blk), 0)
    ti = lax.broadcasted_iota(jnp.int32, (blk, blk), 1)
    upto = jnp.where(si <= ti, 1.0, 0.0).astype(BF16)
    wt = []
    for c in range(2):
        ld = ld_ref[:, c * blk:(c + 1) * blk]
        cat = jnp.concatenate(parts_of(ld, 3), axis=0)
        r = dot(cat, upto)
        gtc = (r[0:nh] + r[nh:2 * nh] + r[2 * nh:3 * nh]) * LOG2E
        gt[:, c * blk:(c + 1) * blk] = gtc
        wt.append(jnp.exp2(gtc[:, blk - 1:blk] - gtc))
    gtv = gt[...]
    g_col = gtv.T
    total = g_col[blk - 1:blk] + g_col[2 * blk - 1:2 * blk]
    tst[...] = jnp.zeros((8, 128), F32)
    tst[0:1, 0:nh] = total

    e3 = one_hot((3 * nh, wid), 64, nh)

    def expand(v, count=3):
        k = count * nh
        return dot(jnp.concatenate(parts_of(v, count), axis=1), e3[0:k] if count < 3 else e3)

    step_col = step_ref[...].T
    w_col = jnp.concatenate(wt, axis=1).T
    e_col = jnp.exp2(g_col)
    state = None
    for c in range(2):
        rows = slice(c * blk, (c + 1) * blk)
        uc = (expand(step_col[rows]) * x_ref[rows].astype(F32)).astype(BF16)
        u[rows] = uc
        wu = (expand(w_col[rows]) * uc.astype(F32)).astype(BF16)
        term = dot(b_ref[rows].T, wu)
        if c == 0:
            s0[...] = term
        else:
            state = expand(e_col[2 * blk - 8:2 * blk])[7:8] * s0[...] + term
    stage[...] = state.astype(BF16)
    pl.semaphore_wait(barrier, 14)

    def slice_of(j):
        return pl.ds(pl.multiple_of(j * 16, 16), 16)

    def a_copy(d):
        j = lax.rem(g + d, 8)
        return pltpu.make_async_remote_copy(
            src_ref=stage.at[slice_of(j)], dst_ref=rs.at[g],
            send_sem=a_send.at[d], recv_sem=a_recv.at[g],
            device_id=at_group(j), device_id_type=MESH)

    def at_copy(d):
        j = lax.rem(g + d, 8)
        return pltpu.make_async_remote_copy(
            src_ref=tst, dst_ref=tr.at[g],
            send_sem=at_send.at[d], recv_sem=at_recv.at[g],
            device_id=at_group(j), device_id_type=MESH)

    def r_copy(d):
        return pltpu.make_async_remote_copy(
            src_ref=rowst, dst_ref=rr.at[row],
            send_sem=r_send.at[d], recv_sem=r_recv.at[row],
            device_id=at_row(lax.rem(row + d, 8)), device_id_type=MESH)

    def rt_copy(d):
        return pltpu.make_async_remote_copy(
            src_ref=rtst, dst_ref=rtr.at[row],
            send_sem=rt_send.at[d], recv_sem=rt_recv.at[row],
            device_id=at_row(lax.rem(row + d, 8)), device_id_type=MESH)

    def c_copy(j):
        return pltpu.make_async_remote_copy(
            src_ref=back.at[j], dst_ref=cin.at[slice_of(g)],
            send_sem=c_send.at[j], recv_sem=c_recv.at[g],
            device_id=at_group(j), device_id_type=MESH)

    def landed(ref, sem):
        pltpu.make_async_copy(ref, ref, sem).wait()

    for d in range(1, 8):
        at_copy(d).start()
    for d in (4, 5, 3, 2, 6, 1, 7):
        a_copy(d).start()
    rs[g] = stage[slice_of(g), :]
    tr[g] = tst[...]
    one3 = one_hot((3 * nh, nh * 128), 128, nh)
    gexp[...] = dot(jnp.concatenate(parts_of(g_col, 3), axis=1), one3)
    eexp[...] = expand(e_col)

    causal = si >= ti

    def local_pairs(c, lo, hi):
        rows = slice(c * blk, (c + 1) * blk)
        cb = lax.dot_general(c_ref[rows], b_ref[rows], (((1,), (1,)), ((), ())),
                             preferred_element_type=F32)
        cb = jnp.where(causal, cb, 0.0)
        lane = lax.broadcasted_iota(jnp.int32, (blk, 128), 1)

        def pair(p, _):
            off = pl.multiple_of(p * 128, 128)
            up = u[rows, pl.ds(off, 128)]
            ys = []
            for k in range(2):
                h = p * 2 + k
                gc = gexp[rows, pl.ds(pl.multiple_of(h * 128, 128), 128)]
                gr = gt[pl.ds(h, 1), rows]
                gap = jnp.concatenate([gc, gc], axis=1) - gr
                m = (jnp.exp2(jnp.minimum(gap, 0.0)) * cb).astype(BF16)
                ys.append(dot(m, up))
            ybuf[rows, pl.ds(off, 128)] = jnp.where(lane < 64, ys[0], ys[1])
            return 0

        lax.fori_loop(lo, hi, pair, 0)

    local_pairs(0, 0, 12)

    for j in range(8):
        @pl.when(j != g)
        def _(j=j):
            landed(tr.at[j], at_recv.at[j])
            landed(rs.at[j], a_recv.at[j])
    e128 = one_hot((128, wid), 64)

    def table(ref):
        t = jnp.concatenate([ref[j, 0:1, :] for j in range(8)], axis=0)
        return t

    def spread(t):
        p = parts_of(t, 3)
        return dot(p[0], e128) + dot(p[1], e128) + dot(p[2], e128)

    tt = table(tr)
    dec = spread(jnp.exp2(tt))
    run = jnp.zeros((16, wid), F32)
    dr = jnp.ones((1, wid), F32)
    for j in range(8):
        pref[j] = run
        dpre[j:j + 1] = dr
        run = run * dec[j:j + 1] + rs[j].astype(F32)
        dr = dr * dec[j:j + 1]
    rowst[...] = run.astype(BF16)
    rtst[...] = jnp.broadcast_to(jnp.sum(tt, axis=0, keepdims=True), (8, 128))
    for d in range(1, 8):
        @pl.when(row + d < 8)
        def _(d=d):
            rt_copy(d).start()
            r_copy(d).start()

    local_pairs(1, 0, 8)

    for r in range(7):
        @pl.when(r < row)
        def _(r=r):
            landed(rtr.at[r], rt_recv.at[r])
            landed(rr.at[r], r_recv.at[r])
    rmask = lax.broadcasted_iota(jnp.int32, (8, 128), 0) < row
    rdec = spread(jnp.where(rmask, jnp.exp2(table(rtr)), 0.0))
    rc = jnp.zeros((16, wid), F32)
    for r in range(7):
        rc = jnp.where(r < row, rc * rdec[r:r + 1] + rr[r].astype(F32), rc)
    for j in range(8):
        back[j] = (pref[j] + dpre[j:j + 1] * rc).astype(BF16)
    for d in (4, 5, 3, 2, 6, 1, 7):
        c_copy(lax.rem(g + d, 8)).start()
    cin[slice_of(g), :] = back[g]

    local_pairs(1, 8, 12)

    skip = expand(jnp.broadcast_to(skip_ref[...], (8, nh)))[0:1]
    et = jnp.where(lax.broadcasted_iota(jnp.int32, (wid, nh), 0) // 64
                   == lax.broadcasted_iota(jnp.int32, (wid, nh), 1), 1.0, 0.0).astype(BF16)
    for j in range(8):
        @pl.when(j != g)
        def _(j=j):
            landed(cin.at[pl.ds(j * 16, 16)], c_recv.at[j])
    entering = cin[...].astype(F32)
    for c in range(2):
        rows = slice(c * blk, (c + 1) * blk)
        if c == 1:
            entering = eexp[blk - 1:blk] * entering + s0[...]
        y = ybuf[rows] + eexp[rows] * dot(c_ref[rows], entering.astype(BF16))
        y = y + skip * x_ref[rows].astype(F32)
        sq = parts_of(y * y, 2)
        ssum = dot(sq[0], et) + dot(sq[1], et)
        inv = lax.rsqrt(ssum * (1.0 / 64.0) + EPSILON)
        n_ref[rows] = (y * expand(inv) * hg_ref[...].reshape(1, wid)).astype(BF16)

    for d in range(1, 8):
        at_copy(d).wait_send()
        a_copy(d).wait_send()
        c_copy(lax.rem(g + d, 8)).wait_send()

        @pl.when(row + d < 8)
        def _(d=d):
            rt_copy(d).wait_send()
            r_copy(d).wait_send()


def mixer(x, b, c, step, ld, skip, hg):
    V = pltpu.VMEM
    D = pltpu.SemaphoreType.DMA
    wid = 1536
    return pl.pallas_call(
        mixer_kernel,
        name="mixer",
        out_shape=jax.ShapeDtypeStruct((512, wid), BF16),
        in_specs=[pl.BlockSpec(memory_space=V)] * 7,
        out_specs=pl.BlockSpec(memory_space=V),
        scratch_shapes=[
            V((512, wid), BF16), V((512, wid), F32), V((512, wid), F32), V((512, 3072), F32),
            V((24, 512), F32), V((128, wid), F32), V((128, wid), BF16), V((8, 16, wid), BF16),
            V((8, 16, wid), F32), V((8, wid), F32), V((16, wid), BF16), V((8, 16, wid), BF16),
            V((8, 16, wid), BF16), V((128, wid), BF16),
            V((8, 128), F32), V((8, 8, 128), F32), V((8, 128), F32), V((8, 8, 128), F32),
        ] + [D((8,))] * 10,
        compiler_params=pltpu.CompilerParams(
            collective_id=1, has_side_effects=True, vmem_limit_bytes=60 * 2**20),
    )(x, b, c, step.T, ld.T, skip.reshape(1, 24), hg)

def back_kernel(n_ref, res_ref, wo_hbm, wq_hbm, gain_ref, stream_ref, out_ref,
                wo_p, wo_o, wq, base, psend, precv, srecv,
                own, buf, knat, osend, oland, mkeep, lkeep, akeep,
                w_sem, p_send, p_recv, s_send, s_recv,
                send_sem, recv_sem, qsend_sem, qrecv_sem, hsend_sem, hrecv_sem, osend_sem, orecv_sem):
    z = lax.axis_index("seq_0")
    yh = lax.axis_index("seq_1")
    xx = lax.axis_index("seq_2")
    cc = lax.axis_index("seq_3")
    tp = lax.axis_index("tp")
    g = xx * 2 + cc
    row = z * 2 + yh
    nrow = lax.rem(row + 1, 8)
    prow = lax.rem(row + 7, 8)
    hd, tok, ch, nch, half = 96, 512, 128, 4, 1536

    def at_group(j):
        return {"seq_2": j // 2, "seq_3": lax.rem(j, 2)}

    def at_row(r):
        return {"seq_0": r // 2, "seq_1": lax.rem(r, 2)}

    partner = {"tp": 1 - tp}
    own_cols = pl.ds(pl.multiple_of(tp * half, half), half)
    far_cols = pl.ds(pl.multiple_of((1 - tp) * half, half), half)

    def dot(a, b):
        return jnp.dot(a, b, preferred_element_type=F32)

    loads = [
        pltpu.make_async_copy(wo_hbm.at[:, far_cols], wo_p, w_sem.at[0]),
        pltpu.make_async_copy(wo_hbm.at[:, own_cols], wo_o, w_sem.at[1]),
        pltpu.make_async_copy(wq_hbm, wq, w_sem.at[2]),
    ]
    for load in loads:
        load.start()

    barrier = pltpu.get_barrier_semaphore()
    for d in range(1, 8):
        pl.semaphore_signal(barrier, inc=1, device_id=at_group(lax.rem(g + d, 8)), device_id_type=MESH)
    for dev in (at_row(nrow), at_row(prow), partner):
        pl.semaphore_signal(barrier, inc=1, device_id=dev, device_id_type=MESH)
    def rows(c):
        return slice(c * ch, (c + 1) * ch)

    def p_copy(c):
        return pltpu.make_async_remote_copy(
            src_ref=psend.at[c], dst_ref=precv.at[c], send_sem=p_send.at[c],
            recv_sem=p_recv.at[c], device_id=partner, device_id_type=MESH)

    def s_copy(c):
        return pltpu.make_async_remote_copy(
            src_ref=stream_ref.at[pl.ds(c * ch, ch)], dst_ref=srecv.at[c], send_sem=s_send.at[c],
            recv_sem=s_recv.at[c], device_id=partner, device_id_type=MESH)

    def project(c):
        psend[c] = dot(n_ref[rows(c)], wo_p[...]).astype(BF16)

    def add_up(c):
        p_copy(c).wait_recv()
        stream_ref[rows(c)] = (base[rows(c)] + precv[c].astype(F32)).astype(BF16)
        s_copy(c).start()

    loads[0].wait()
    project(0)
    pl.semaphore_wait(barrier, 10)
    p_copy(0).start()
    project(1)
    p_copy(1).start()
    loads[1].wait()
    for c in range(nch):
        base[rows(c)] = res_ref[rows(c)].astype(F32) + dot(n_ref[rows(c)], wo_o[...])
    project(2)
    project(3)
    for c in range(2):
        add_up(c)
        p_copy(c + 2).start()
    loads[2].wait()

    def head(j):
        return pl.ds(pl.multiple_of(j * hd, 32), hd)

    def kv_copy(c, d):
        j = lax.rem(g + d, 8)
        return pltpu.make_async_remote_copy(
            src_ref=own.at[c, pl.ds(1, 2), head(j), :],
            dst_ref=buf.at[4 + g, c, pl.ds(1, 2)],
            send_sem=send_sem.at[c, d],
            recv_sem=recv_sem.at[c, g],
            device_id=at_group(j), device_id_type=MESH)

    def q_copy(c, d):
        j = lax.rem(g + d, 8)
        return pltpu.make_async_remote_copy(
            src_ref=own.at[c, 0, head(j), :],
            dst_ref=buf.at[4 + g, c, 0],
            send_sem=qsend_sem.at[c, d],
            recv_sem=qrecv_sem.at[c, g],
            device_id=at_group(j), device_id_type=MESH)

    def halo_copy(c, i):
        return pltpu.make_async_remote_copy(
            src_ref=buf.at[8 + i, c, pl.ds(1, 2)],
            dst_ref=buf.at[i, c, pl.ds(1, 2)],
            send_sem=hsend_sem.at[c, i],
            recv_sem=hrecv_sem.at[c, i],
            device_id=at_row(nrow), device_id_type=MESH)

    def out_copy(b):
        return pltpu.make_async_remote_copy(
            src_ref=osend.at[b],
            dst_ref=oland.at[g],
            send_sem=osend_sem.at[b],
            recv_sem=orecv_sem.at[g],
            device_id=at_group(b), device_id_type=MESH)

    def landed(ref, sem):
        pltpu.make_async_copy(ref, ref, sem).wait()

    def arrivals(c):
        for b in (7, 6, 5, 4, 0, 1, 2, 3):
            @pl.when(b != g)
            def _(b=b):
                landed(buf.at[4 + b, c, pl.ds(1, 2)], recv_sem.at[c, b])
            if b >= 4:
                @pl.when(row < 7)
                def _(b=b):
                    halo_copy(c, b - 4).start()
        for b in range(8):
            knat[4 + b, c * ch:(c + 1) * ch, :] = buf[4 + b, c, 1].T
        for b in range(8):
            @pl.when(b != g)
            def _(b=b):
                landed(buf.at[4 + b, c, 0], qrecv_sem.at[c, b])

    scale = (hd ** -0.5) * LOG2E
    early = 2 * ch
    low = (lax.broadcasted_iota(jnp.int32, (early, early), 0)
           <= lax.broadcasted_iota(jnp.int32, (early, early), 1))

    def wide(j, i, lo, hi):
        return jnp.concatenate([buf[j, c, i] for c in range(lo, hi)], axis=1)

    @pl.when(row == 0)
    def _():
        for i in range(4):
            knat[i] = jnp.zeros((tok, hd), BF16)
            for c in range(nch):
                buf[i, c, 2] = jnp.zeros((hd, ch), BF16)

    def order(step):
        return jnp.where(step < 4, 4 + step, 7 - step)

    def halo_in(step, b, lo, hi):
        @pl.when(jnp.logical_and(step >= 4, row > 0))
        def _():
            for c in range(lo, hi):
                halo_copy(c, b).wait_recv()
                knat[b, c * ch:(c + 1) * ch, :] = buf[b, c, 1].T

    def top(tiles):
        m = None
        for t, ok in tiles:
            r = jnp.max(t, axis=0, keepdims=True)
            if ok is not None:
                r = jnp.where(ok, r, NEG)
            m = r if m is None else jnp.maximum(m, r)
        return m

    def powers(tiles, m):
        ps = [jnp.exp2(t - (m if ok is None else jnp.where(ok, m, -NEG))) for t, ok in tiles]
        l = jnp.sum(ps[0], axis=0, keepdims=True)
        for t in ps[1:]:
            l = l + jnp.sum(t, axis=0, keepdims=True)
        return ps, l

    def square(b, lo, hi, qt, far):
        s_diag = dot(knat[4 + b, lo:hi], qt)
        s_far = dot(knat[b, lo:hi], qt)
        return jnp.where(low, s_diag, jnp.where(far, s_far, NEG))

    def halves(p):
        return [jnp.where(low, p, 0.0).astype(BF16), jnp.where(low, 0.0, p).astype(BF16)]

    def there(b, i):
        return jnp.logical_or(b + i >= 4, row > 0)

    def first_round(step, _):
        b = order(step)
        halo_in(step, b, 0, 2)
        qt = wide(4 + b, 0, 0, 2)
        tiles = [(square(b, 0, early, qt, there(b, 0)), None)]
        tiles += [(dot(knat[b + i, 0:early], qt), there(b, i)) for i in range(1, 4)]
        m = top(tiles)
        ps, l = powers(tiles, m)
        pt = jnp.concatenate(halves(ps[0]) + [t.astype(BF16) for t in ps[1:]], axis=0)
        vt = jnp.concatenate([wide(j, 2, 0, 2) for j in (4 + b, b, b + 1, b + 2, b + 3)], axis=1)
        mkeep[b] = m
        lkeep[b] = l
        akeep[b] = dot(vt, pt)
        return 0

    def second_round(step, _):
        b = order(step)
        halo_in(step, b, 2, 4)

        qt = wide(4 + b, 0, 0, 2)
        tiles = [(dot(knat[b + i, early:tok], qt), there(b, i)) for i in range(4)]
        m = mkeep[b]
        m_new = jnp.maximum(m, top(tiles))
        alpha = jnp.exp2(m - m_new)
        ps, l = powers(tiles, m_new)
        l = alpha * lkeep[b] + l
        pt = jnp.concatenate([t.astype(BF16) for t in ps], axis=0)
        vt = jnp.concatenate([wide(b + i, 2, 2, 4) for i in range(4)], axis=1)
        osend[b, :, 0:early] = ((alpha * akeep[b] + dot(vt, pt)) / l).astype(BF16)

        qt = wide(4 + b, 0, 2, 4)
        tiles = [(square(b, early, tok, qt, there(b, 0)), None), (dot(knat[4 + b, 0:early], qt), None)]
        tiles += [(dot(knat[b + i], qt), there(b, i)) for i in range(1, 4)]
        ps, l = powers(tiles, top(tiles))
        pt = jnp.concatenate(halves(ps[0]) + [t.astype(BF16) for t in ps[1:]], axis=0)
        vt = jnp.concatenate(
            [wide(4 + b, 2, 2, 4), wide(b, 2, 2, 4), wide(4 + b, 2, 0, 2)]
            + [wide(b + i, 2, 0, 4) for i in range(1, 4)], axis=1)
        osend[b, :, early:tok] = (dot(vt, pt) / l).astype(BF16)

        @pl.when(b != g)
        def _():
            out_copy(b).start()
        return 0

    gain_own = gain_ref[own_cols].reshape(1, half)
    gain_far = gain_ref[far_cols].reshape(1, half)
    for c in range(nch):
        landed(srecv.at[c], s_recv.at[c])
        a = stream_ref[rows(c)].astype(F32)
        f = srecv[c].astype(F32)
        ss = jnp.sum(a * a, axis=1, keepdims=True) + jnp.sum(f * f, axis=1, keepdims=True)
        inv = lax.rsqrt(ss * (1.0 / (2 * half)) + EPSILON)
        na = (a * inv * gain_own).astype(BF16)
        nf = (f * inv * gain_far).astype(BF16)
        for i in (1, 2, 0):
            r = dot(na, wq[i, own_cols, :]) + dot(nf, wq[i, far_cols, :])
            if i == 0:
                r = r * scale
            own[c, i] = r.astype(BF16).T
            for d in (4, 5, 3, 2, 6, 1, 7):
                if i == 2:
                    kv_copy(c, d).start()
                if i == 0:
                    q_copy(c, d).start()
        buf[4 + g, c] = own[c, :, head(g), :]
        if c < 2:
            add_up(c + 2)
        if c > 0:
            arrivals(c - 1)
        if c == 2:
            lax.fori_loop(0, 4, first_round, 0)
        if c == 3:
            lax.fori_loop(4, 8, first_round, 0)
    arrivals(nch - 1)
    lax.fori_loop(0, 8, second_round, 0)
    oland[g] = osend[g]
    for b in range(8):
        @pl.when(b != g)
        def _(b=b):
            landed(oland.at[b], orecv_sem.at[b])
    out_ref[...] = oland[...].reshape(8 * hd, tok).T
    for c in range(nch):
        p_copy(c).wait_send()
        s_copy(c).wait_send()
        for d in range(1, 8):
            kv_copy(c, d).wait_send()
            q_copy(c, d).wait_send()
    for b in range(8):
        @pl.when(b != g)
        def _(b=b):
            out_copy(b).wait_send()

    @pl.when(row < 7)
    def _():
        for c in range(nch):
            for i in range(4):
                halo_copy(c, i).wait_send()


def back(normed, residual, mixer_out, weight, gain):
    V = pltpu.VMEM
    D = pltpu.SemaphoreType.DMA
    vm = pl.BlockSpec(memory_space=V)
    hbm = pl.BlockSpec(memory_space=pl.ANY)
    return pl.pallas_call(
        back_kernel,
        name="back",
        out_shape=(jax.ShapeDtypeStruct((512, 1536), BF16), jax.ShapeDtypeStruct((512, 768), BF16)),
        in_specs=[vm, vm, hbm, hbm, vm],
        out_specs=(vm, vm),
        scratch_shapes=[
            V((1536, 1536), BF16), V((1536, 1536), BF16), V((3, 3072, 768), BF16),
            V((512, 1536), F32), V((4, 128, 1536), BF16), V((4, 128, 1536), BF16), V((4, 128, 1536), BF16),
            V((4, 3, 768, 128), BF16), V((12, 4, 3, 96, 128), BF16), V((12, 512, 96), BF16),
            V((8, 96, 512), BF16), V((8, 96, 512), BF16),
            V((8, 1, 256), F32), V((8, 1, 256), F32), V((8, 96, 256), F32),
            D((3,)), D((4,)), D((4,)), D((4,)), D((4,)),
            D((4, 8)), D((4, 8)), D((4, 8)), D((4, 8)), D((4, 4)), D((4, 4)), D((8,)), D((8,)),
        ],
        compiler_params=pltpu.CompilerParams(
            collective_id=2, has_side_effects=True, vmem_limit_bytes=54 * 2**20),
    )(normed, residual, mixer_out, weight, gain)


def on_device(
    mixer_input,
    state_write,
    state_read,
    step_size,
    log_decay,
    skip_gain,
    head_gain,
    mixer_out,
    residual,
    attn_gain,
    qkv_weight,
):
    normed = mixer(mixer_input, state_write, state_read, step_size, log_decay, skip_gain, head_gain)
    weight = jnp.transpose(qkv_weight, (1, 0, 2))
    stream, pieces = back(normed, residual, mixer_out, weight, attn_gain)
    return (stream, pieces)


def solution(mesh):
    torus = Mesh(
        mesh.devices.reshape(4, 2, 4, 2, mesh.shape["tp"]),
        ("seq_0", "seq_1", "seq_2", "seq_3", "tp"),
    )
    in_specs = (
        P(SEQ, "tp"),
        P(SEQ, None),
        P(SEQ, None),
        P(SEQ, "tp"),
        P(SEQ, "tp"),
        P("tp"),
        P("tp"),
        P("tp", None),
        P(SEQ, "tp"),
        P(),
        P(None, None, "tp"),
    )
    out_specs = (P(SEQ, "tp"), P(SEQ, "tp"))
    return jax.shard_map(
        on_device, mesh=torus, in_specs=in_specs, out_specs=out_specs, check_vma=False
    )
```
